32 devices in a mesh: groups: 2 (over x), sph: 16 (over z, y, core).
Axes of the slice: x: 2, y: 2, z: 4, core: 2. Of those that a mesh axis runs over, the one named last changes fastest.
Arguments:
- positions: float32 [512, 3], P('sph'), may hold values from -8 to 8
- wave_vectors: float32 [256, 3], replicated, may hold values from -5 to 5
- pattern: float32 [2, 448, 256], replicated, may hold values from -6 to 6
- dir_index: int32 [64], P('groups'), parts along dimension 0, may hold values from 0 to 255
- mie: float32 [2, 448, 512], P(None, None, 'sph'), may hold values from -0.9 to 0.9
- trans_table: bfloat16 [8, 2, 448, 448], replicated, may hold values from -0.1875 to 0.1875
- pair_route: int32 [1024, 1], P('sph'), may hold values from 0 to 15; in each aligned block of 64 rows (0 to 63, 64 to 127, ...) at most 8 rows name the same one
- pair_source: int32 [1024], P('sph'), may hold values from 0 to 15
- pair_target: int32 [1024], P('sph'), may hold values from 0 to 15
- pair_class: int32 [1024], P('sph'), may hold values from 0 to 7
Outputs:
- scattered: bfloat16 [896, 32768], P(None, ('groups', 'sph')), parts along dimension 1
- extinction: float32 [64], P('groups'), parts along dimension 0
The draws below stay inside these ranges and needn't reach their ends.
There are 2 independent parts, one for each index of `groups`. The reference program is written for one: setup_inputs(seed, part) draws one part's arguments, and reference() takes and returns one part's arrays. A program takes and returns all parts, laid end to end along the dimension named above; an argument that names none is the same for every part. Nothing has to cross between parts.
Inputs may be any that keep to these rules, and one draw needn't show every extreme that they name: `pair_route`: among the rows of one device no device is named by more than 8 pairs, and in every draw some device is named by exactly 8 of them.
All inputs are finite; a program needn't handle non-finite values.
Results may differ from the reference program's by a relative error of at most 0.0051.
Values may be sent and summed in bfloat16 or wider, within the bound.
A program may use at most 192 MiB of HBM per device.

```python
import math
import jax
import jax.numpy as jnp
import numpy as np
from jax import lax

MODES = 448
DIRS = 32
DIRTAB = 256
CLASSES = 8
BLOCK = 2
BLK_DEV = 16
PAIRS_DEV = 64
CAP = 8
SPHERES = 512
PAIRS = 1024
N_SPH = 16


def place_ends(drawn, key, smallest, high):
    extent = drawn.shape
    index_at = [jax.random.randint(jax.random.fold_in(key, axis), (), 0, extent[axis]) for axis in range(len(extent))]
    drawn = drawn.at[tuple(index_at)].set(smallest)
    longest = extent.index(max(extent))
    index_at[longest] = (index_at[longest] + 1) % extent[longest]
    return drawn.at[tuple(index_at)].set(high)


def shard_levels(stream_key, shape, shards, smallest, top_value):
    factor_of = 1.0
    for axis_at, shards_of in shards:
        heights = jax.random.uniform(jax.random.fold_in(jax.random.fold_in(stream_key, 6), axis_at), (shards_of,), jnp.float32, smallest / len(shards), top_value / len(shards))
        factor_of = factor_of * jnp.repeat(jnp.exp(heights), shape[axis_at] // shards_of).reshape((-1,) + (1,) * (len(shape) - 1 - axis_at))
    return factor_of


def shared_out(own_key, own, number, rows, number_of, top, bound, lean):
    order = jax.random.permutation(own_key, number_of)
    crowded, common = load_shares(number_of, rows * top, bound, lean, True), load_shares(number_of, rows * top, bound, lean, False)
    places = jnp.arange(number_of)

    def named(tallies, offset_by):
        used = int((tallies > 0).sum())
        fixed = max(1, used // 4)
        shifted = fixed + (places - fixed + offset_by * (used - fixed)) % max(1, number_of - fixed)
        return jnp.zeros((number_of,), jnp.int32).at[order[jnp.where(places < fixed, places, shifted)]].set(jnp.asarray(tallies, jnp.int32))

    tallies = jnp.where(number % 4 == 0, named(crowded, number // 4), named(common, number - number // 4 - 1))
    mixed = jax.random.permutation(jax.random.fold_in(own, 3), number_of)
    giver, sink = mixed[0:number_of // 2 * 2:2], mixed[1:number_of // 2 * 2:2]
    slack = jnp.minimum(tallies[giver] - 1, bound - tallies[sink]) // 2
    slack = jnp.where((giver == order[0]) | (sink == order[0]) | (tallies[sink] == 0), 0, jnp.maximum(slack, 0))
    shifted = jax.random.randint(jax.random.fold_in(own, 4), (number_of // 2,), 0, 1 << 20) % (slack + 1)
    tallies = tallies.at[giver].add(-shifted).at[sink].add(shifted)
    items = jnp.searchsorted(jnp.cumsum(tallies), jnp.arange(rows * top), side="right").astype(jnp.int32)
    table = items.reshape(top, rows).T
    table = table[jax.random.permutation(jax.random.fold_in(own, 1), rows)]
    offset_by = jax.random.randint(jax.random.fold_in(own, 2), (rows, 1), 0, top)
    return jnp.take_along_axis(table, (jnp.arange(top)[None, :] + offset_by) % top, axis=1)


def load_shares(count, total, bound, skew, full):
    portions = [(1 << 20) // math.isqrt(rank ** skew) + 1 for rank in range(1, count + 1)]
    largest = bound if full else min(bound, max(-(-total // count), total * portions[0] // sum(portions)))
    least = 1 if total - largest >= count - 1 else 0
    given, rest = [largest] + [least] * (count - 1), total - largest - least * (count - 1)
    while rest > 0:
        candidates = [i for i in range(1, count) if given[i] < largest] or [i for i in range(1, count) if given[i] < bound]
        pool, budget = sum([portions[i] for i in candidates]), rest
        for i in candidates:
            addition = min(bound - given[i], max(1, budget * portions[i] // pool), rest)
            given[i] = given[i] + addition
            rest = rest - addition
    return np.array(given)


def gaussian(key, shape, scale, most, kind=jnp.bfloat16):
    return jnp.clip(scale * jax.random.normal(key, shape, jnp.float32), -most, most).astype(kind)


def setup_inputs(seed: int = 0, part: int = 0) -> dict:
    key_list = jax.random.split(jax.random.key(seed), 11)
    part_splits = jax.random.split(jax.random.fold_in(key_list[10], part), 11)
    positions = jnp.clip(jax.random.uniform(key_list[0], (SPHERES, 3), jnp.float32, -8.0, 8.0) * shard_levels(key_list[0], (SPHERES, 3), ((0, 16),), -0.4, 0.0), -8.0, 8.0)
    wave_vectors = gaussian(key_list[1], (DIRTAB, 3), 1.0, 5.0, jnp.float32)
    pattern = gaussian(key_list[2], (2, MODES, DIRTAB), 1.0, 6.0, jnp.float32)
    dir_index = place_ends(jax.random.randint(part_splits[3], (DIRS,), 0, DIRTAB), jax.random.fold_in(part_splits[3], 1), 0, DIRTAB - 1).astype(jnp.int32)
    mie = jnp.clip(jax.random.uniform(key_list[4], (2, MODES, SPHERES), jnp.float32, -0.9, 0.9) * shard_levels(key_list[4], (2, MODES, SPHERES), ((2, 16),), -0.4, 0.0), -0.9, 0.9)
    trans_table = gaussian(key_list[5], (CLASSES, 2, MODES, MODES), (2 * MODES) ** -0.5, 0.1875)
    pair_route_keys = jax.random.split(jax.random.fold_in(key_list[6], 1), PAIRS // PAIRS_DEV)
    pair_route_turns = jax.random.permutation(jax.random.fold_in(key_list[6], 3), PAIRS // PAIRS_DEV)
    pair_route = jax.vmap(lambda own, number: shared_out(jax.random.fold_in(key_list[6], 2), own, number, PAIRS_DEV, N_SPH, 1, CAP, 2))(pair_route_keys, pair_route_turns).reshape((PAIRS, 1))
    pair_source = place_ends(jax.random.randint(key_list[7], (PAIRS,), 0, BLK_DEV), jax.random.fold_in(key_list[7], 1), 0, BLK_DEV - 1).astype(jnp.int32)
    pair_target = place_ends(jax.random.randint(key_list[8], (PAIRS,), 0, BLK_DEV), jax.random.fold_in(key_list[8], 1), 0, BLK_DEV - 1).astype(jnp.int32)
    pair_class = place_ends(jax.random.randint(key_list[9], (PAIRS,), 0, CLASSES), jax.random.fold_in(key_list[9], 1), 0, CLASSES - 1).astype(jnp.int32)
    return dict(positions=positions, wave_vectors=wave_vectors, pattern=pattern, dir_index=dir_index, mie=mie, trans_table=trans_table, pair_route=pair_route, pair_source=pair_source, pair_target=pair_target, pair_class=pair_class)


def reference(positions, wave_vectors, pattern, dir_index, mie, trans_table, pair_route, pair_source, pair_target, pair_class):
    directions = wave_vectors[dir_index]
    phases = positions[:, 0:1] * directions[None, :, 0] + positions[:, 1:2] * directions[None, :, 1] + positions[:, 2:3] * directions[None, :, 2]
    cosine = jnp.cos(phases)
    sine_part = jnp.sin(phases)
    chosen = pattern[:, :, dir_index]
    inc_real = cosine[None] * chosen[0][:, None, :] - sine_part[None] * chosen[1][:, None, :]
    inc_imag = cosine[None] * chosen[1][:, None, :] + sine_part[None] * chosen[0][:, None, :]
    mie_real = mie[0][:, :, None]
    mie_imag = mie[1][:, :, None]
    scat_real = mie_real * inc_real - mie_imag * inc_imag
    scat_imag = mie_real * inc_imag + mie_imag * inc_real
    coeffs = jnp.concatenate([scat_real, scat_imag], 0).astype(jnp.bfloat16)
    columns = BLOCK * DIRS
    block_count = SPHERES // BLOCK
    block_data = coeffs.reshape(2 * MODES, block_count, columns).transpose(1, 0, 2)
    owner = jnp.arange(PAIRS, dtype=jnp.int32) // PAIRS_DEV
    source_global = (owner * BLK_DEV + pair_source).astype(jnp.int32)
    target_global = (pair_route[:, 0] * BLK_DEV + pair_target).astype(jnp.int32)
    group_shape = (PAIRS // 8, 8)

    def add_group(field_sum, group_items):
        sources, targets, classes = group_items
        tables = trans_table[classes].astype(jnp.float32)
        values = block_data[sources].astype(jnp.float32)
        data_real = values[:, :MODES]
        data_imag = values[:, MODES:]
        highest = lax.Precision.HIGHEST
        part_real = jnp.einsum('kij,kjc->kic', tables[:, 0], data_real, precision=highest) - jnp.einsum('kij,kjc->kic', tables[:, 1], data_imag, precision=highest)
        part_imag = jnp.einsum('kij,kjc->kic', tables[:, 1], data_real, precision=highest) + jnp.einsum('kij,kjc->kic', tables[:, 0], data_imag, precision=highest)
        contribution = jnp.concatenate([part_real, part_imag], 1).astype(jnp.bfloat16)
        contribution = lax.optimization_barrier(contribution).astype(jnp.float32)
        return field_sum.at[targets].add(contribution), None

    initial = jnp.zeros((block_count, 2 * MODES, columns), jnp.float32)
    summed, unused = lax.scan(add_group, initial, (source_global.reshape(group_shape), target_global.reshape(group_shape), pair_class.astype(jnp.int32).reshape(group_shape)))
    summed = summed.transpose(1, 0, 2).reshape(2 * MODES, SPHERES, DIRS)
    total_real = inc_real + summed[:MODES]
    total_imag = inc_imag + summed[MODES:]
    out_real = mie_real * total_real - mie_imag * total_imag
    out_imag = mie_real * total_imag + mie_imag * total_real
    scattered = jnp.concatenate([out_real, out_imag], 0).reshape(2 * MODES, SPHERES * DIRS).astype(jnp.bfloat16)
    extinction = jnp.sum(inc_real * out_real + inc_imag * out_imag, axis=(0, 1))
    return (scattered, extinction)
```

```python
import functools

import jax
import jax.numpy as jnp
from jax import lax
from jax.experimental import pallas as pl
from jax.experimental.pallas import tpu as pltpu
from jax.sharding import PartitionSpec as P

BLOCK = 2
LANES = 128
HIGHEST = lax.Precision.HIGHEST
MESH = pl.DeviceIdType.MESH
F32 = jnp.float32
BF16 = jnp.bfloat16
ORDER = ((0, 2, 1, 3), (3, 0, 2, 1))


def sincos(angle):
    turns = jnp.floor(angle * 0.6366197723675814 + 0.5)
    rest = angle - turns * 1.5703125
    rest = rest - turns * 4.837512969970703125e-4
    rest = rest - turns * 7.54978995489188216e-8
    square = rest * rest
    sine = rest + rest * square * (
        -1.6666654611e-1 + square * (8.3321608736e-3 + square * -1.9515295891e-4)
    )
    cosine = 1.0 - 0.5 * square + square * square * (
        4.166664568298827e-2 + square * (-1.388731625493765e-3 + square * 2.443315711809948e-5)
    )
    quarter = turns.astype(jnp.int32)
    swap = (quarter & 1) == 1
    c = jnp.where(swap, sine, cosine)
    s = jnp.where(swap, cosine, sine)
    c = jnp.where(((quarter + 1) & 2) == 2, -c, c)
    s = jnp.where((quarter & 2) == 2, -s, s)
    return c, s


def split_two(x):
    high = x.astype(BF16)
    return high, (x - high.astype(F32)).astype(BF16)


def fused_kernel(
    dims, route, source, target, kind, pos_s, pos_v, wave_s, dir_s, mie, pattern_hbm, table_hbm,
    scattered, ext,
    table, pattern, t_real, t_diff, t_sum, all_mie, all_small, weights, x_real, x_imag, x_sum,
    pat, inc, spread, own_e, phase, delta, y_at, out_at, part, inbox,
    loaded, stored, send, recv, ext_send, ext_recv,
):
    modes, dirs, spheres, blocks, classes, devices, capacity = dims
    me = lax.axis_index("sph")
    chips = devices // 2
    chip, core = me // 2, me % 2
    other = chip * 2 + (1 - core)
    bits = []
    bit = chips // 2
    while bit >= 1:
        bits.append(bit)
        bit //= 2

    def flip(value, bit):
        return value + bit - 2 * bit * ((value // bit) % 2)

    partners = [flip(chip, bit) * 2 + core for bit in bits] + [other]
    everyone = [(me + r) % devices for r in range(1, devices)]

    barrier = pltpu.get_barrier_semaphore()
    for peer in partners:
        pl.semaphore_signal(barrier, inc=1, device_id={"sph": peer}, device_id_type=MESH)
    load_table = pltpu.make_async_copy(table_hbm, table, loaded.at[0])
    load_pattern = pltpu.make_async_copy(pattern_hbm, pattern, loaded.at[1])
    load_table.start()
    load_pattern.start()

    pairs = route.shape[1]
    slots = devices * capacity
    ia = lax.broadcasted_iota(jnp.int32, (pairs, pairs), 0)
    ib = lax.broadcasted_iota(jnp.int32, (pairs, pairs), 1)

    def column(row):
        return jnp.sum(jnp.where(ia == ib, row, 0.0), 1, keepdims=True)

    dest = route[...].astype(F32)
    dest_col = column(dest)
    rank = jnp.sum(jnp.where((dest_col == dest) & (ib < ia), 1.0, 0.0), 1, keepdims=True)
    slot_lane = lax.broadcasted_iota(jnp.int32, (pairs, LANES), 1).astype(F32)
    match = (dest_col * capacity + rank) == slot_lane
    source_col = column(source[...].astype(F32))
    cell_col = column((kind[...] * blocks + target[...] + 1).astype(F32))
    sphere_lane = lax.broadcasted_iota(jnp.int32, (pairs, spheres), 1).astype(F32)
    entries = [cell_col, source_col]
    for j in range(BLOCK):
        picked = sphere_lane == source_col * BLOCK + j
        for axis in range(3):
            entries.append(
                jnp.sum(jnp.where(picked, pos_v[axis : axis + 1, :], 0.0), 1, keepdims=True)
            )
    rows = [jnp.sum(jnp.where(match, entry, 0.0), 0, keepdims=True) for entry in entries]
    all_small[me] = jnp.concatenate(rows, 0)
    all_mie[me] = jnp.concatenate([mie[0], mie[1]], 1).astype(BF16)

    pl.semaphore_wait(barrier, len(partners))

    copies = []

    def start(origin, mask, step):
        slot = mask if step == len(bits) else mask + bits[step]
        slot = slot + chips if step == len(bits) else slot
        back = chips * step + mask
        for at, ref in ((0, all_small), (1, all_mie)):
            copy = pltpu.make_async_remote_copy(
                src_ref=ref.at[origin], dst_ref=ref.at[origin],
                send_sem=send.at[at, back], recv_sem=recv.at[at, slot],
                device_id={"sph": partners[step]}, device_id_type=MESH,
            )
            copy.start()
            copies.append(copy)

    def arrived(at, slot):
        ref = (all_small, all_mie)[at]
        pltpu.make_async_remote_copy(
            src_ref=ref.at[me], dst_ref=ref.at[me],
            send_sem=send.at[at, 0], recv_sem=recv.at[at, slot],
            device_id={"sph": other}, device_id_type=MESH,
        ).wait_recv()

    def low(mask):
        return mask & -mask

    def origin_of(mask):
        value = chip
        for bit in bits:
            if mask & bit:
                value = flip(value, bit)
        return value * 2 + core

    for step in range(len(bits) + 1):
        start(me, 0, step)

    def forward(mask):
        arrived(0, mask)
        arrived(1, mask)
        for step, bit in enumerate(bits):
            if bit < low(mask):
                start(origin_of(mask), mask, step)
        start(origin_of(mask), mask, len(bits))

    waits = sorted(range(1, chips), key=lambda mask: (bin(mask).count("1"), -mask))

    per = LANES // dirs
    lane = lax.broadcasted_iota(jnp.int32, (1, LANES), 1)
    group = lane // dirs
    k_rows = []
    dir_row = jnp.zeros((1, LANES), jnp.int32)
    for axis in range(3):
        k_rows.append(jnp.zeros((1, LANES), F32))
    for d in range(dirs):
        here = lane % dirs == d
        index = dir_s[d]
        dir_row = jnp.where(here, index, dir_row)
        for axis in range(3):
            k_rows[axis] = jnp.where(here, wave_s[axis, index], k_rows[axis])

    def block_of(j):
        order = jnp.zeros((1, LANES), jnp.int32)
        for g in range(per):
            order = jnp.where(group == g, ORDER[j][g], order)
        return order

    orders = [block_of(j) for j in range(BLOCK)]
    steps = blocks // per
    tiles = [(q, j) for q in range(steps) for j in range(BLOCK)]
    sphere_at = jnp.concatenate([(orders[j] + q * per) * BLOCK + j for q, j in tiles], 0)
    here = [jnp.zeros((len(tiles), LANES), F32) for _ in range(3)]
    for s in range(spheres):
        mine = sphere_at == s
        for axis in range(3):
            here[axis] = jnp.where(mine, pos_s[axis, s], here[axis])

    def phase_of(x, y, z):
        return sincos(x * k_rows[0] + y * k_rows[1] + z * k_rows[2])

    own_c, own_s = phase_of(*here)
    own_e[0] = own_c
    own_e[1] = own_s

    def prepare_table():
        load_table.wait()
        for c in range(0, classes, 2):
            at = pl.ds(c * modes, 2 * modes)
            real = jnp.concatenate([table[c, 0], table[c + 1, 0]], 1)
            imag = jnp.concatenate([table[c, 1], table[c + 1, 1]], 1)
            t_real[:, at] = real
            t_diff[:, at] = imag - real
            t_sum[:, at] = imag + real

    def prepare_field():
        load_pattern.wait()
        tables = pattern.shape[2]
        chosen = (lax.broadcasted_iota(jnp.int32, (tables, LANES), 0) == dir_row).astype(F32).astype(BF16)
        for p in range(2):
            high, rest = split_two(pattern[p])
            pat[p] = jnp.dot(high, chosen, preferred_element_type=F32) + jnp.dot(
                rest, chosen, preferred_element_type=F32
            )
        sphere_id = lax.broadcasted_iota(jnp.int32, (spheres, LANES), 0)
        picks = jnp.concatenate(
            [(sphere_id == sphere_at[t : t + 1]).astype(F32) for t in range(len(tiles))], 1
        )
        picks = jnp.concatenate([picks, picks], 0).astype(BF16)
        for p in range(2):
            pieces = jnp.concatenate(split_two(mie[p]), 0)
            spread[p] = lax.dot_general(
                pieces, picks, (((0,), (0,)), ((), ())), preferred_element_type=F32
            )
        for t in range(len(tiles)):
            at = pl.ds(t * LANES, LANES)
            c, s = own_c[t : t + 1], own_s[t : t + 1]
            inc[0, :, at] = c * pat[0] - s * pat[1]
            inc[1, :, at] = c * pat[1] + s * pat[0]

    for mask in waits[:1]:
        forward(mask)
    prepare_table()
    for mask in waits[1:3]:
        forward(mask)
    prepare_field()
    for mask in waits[3:]:
        forward(mask)
    for slot in range(chips):
        arrived(0, chips + slot)

    slot_id = lax.broadcasted_iota(jnp.int32, (slots, devices), 0)
    from_device = (slot_id // capacity == lax.broadcasted_iota(jnp.int32, (slots, devices), 1)).astype(F32)
    lists = jnp.concatenate([all_small[:, r, :] for r in range(8)], 1)
    lists = jnp.dot(from_device, lists, precision=HIGHEST, preferred_element_type=F32)
    slot_row = lax.broadcasted_iota(jnp.int32, (slots, LANES), 0)
    slot_lane = lax.broadcasted_iota(jnp.int32, (slots, LANES), 1)
    wanted = slot_lane == me * capacity + slot_row % capacity
    cols = [
        jnp.sum(jnp.where(wanted, lists[:, r * LANES : (r + 1) * LANES], 0.0), 1, keepdims=True)
        for r in range(8)
    ]
    cell = cols[0].astype(jnp.int32) - 1
    owner = lax.broadcasted_iota(jnp.int32, (slots, 1), 0) // capacity
    row_of = owner * spheres + cols[1].astype(jnp.int32) * BLOCK
    for j in range(BLOCK):
        c, s = phase_of(*cols[2 + 3 * j : 5 + 3 * j])
        phase[j, :slots, :] = c
        phase[j, slots:, :] = s
        delta[j] = cell - orders[j]
    total = devices * spheres
    at_row = lax.broadcasted_iota(jnp.int32, (slots, total), 1)
    pick = jnp.concatenate(
        [(at_row == row_of + j).astype(F32).astype(BF16) for j in range(BLOCK)], 0
    )

    for slot in range(chips):
        arrived(1, chips + slot)
    gathered = jnp.dot(
        pick, all_mie[...].reshape(total, 2 * modes), preferred_element_type=F32
    )
    for j in range(BLOCK):
        turned = gathered[j * slots : (j + 1) * slots].T.astype(BF16)
        real, imag = turned[:modes], turned[modes:]
        weights[j, :modes, :slots] = real
        weights[j, modes:, :slots] = imag
        weights[j, :modes, slots:] = -imag
        weights[j, modes:, slots:] = real

    width = BLOCK * LANES

    def step_body(q, carry):
        for j in range(BLOCK):
            c_all, s_all = phase[j, :slots, :], phase[j, slots:, :]
            for c in range(0, classes, 2):
                tops, bottoms = [], []
                for h in range(2):
                    here = delta[j] == (c + h) * blocks + q * per
                    tops.append(jnp.where(here, c_all, 0.0))
                    bottoms.append(jnp.where(here, s_all, 0.0))
                masked = jnp.concatenate(
                    [jnp.concatenate(tops, 1), jnp.concatenate(bottoms, 1)], 0
                ).astype(BF16)
                y_at[...] = jnp.dot(weights[j], masked, preferred_element_type=F32)
                for h in range(2):
                    at = pl.ds(h * LANES, LANES)
                    yr, yi = y_at[:modes, at], y_at[modes:, at]
                    pr, pi = pat[0], pat[1]
                    mr = yr * pr - yi * pi
                    mi = yr * pi + yi * pr
                    rows = pl.ds((c + h) * modes, modes)
                    lanes = pl.ds(j * LANES, LANES)
                    x_real[rows, lanes] = mr.astype(BF16)
                    x_imag[rows, lanes] = mi.astype(BF16)
                    x_sum[rows, lanes] = (mr + mi).astype(BF16)
        both = jnp.dot(t_real[...], x_sum[...], preferred_element_type=F32)
        first = jnp.dot(t_diff[...], x_real[...], preferred_element_type=F32)
        second = jnp.dot(t_sum[...], x_imag[...], preferred_element_type=F32)
        at = pl.ds(pl.multiple_of(q * width, width), width)
        inc_r, inc_i = inc[0, :, at], inc[1, :, at]
        total_r = inc_r + (both - second)
        total_i = inc_i + (both + first)
        mr, mi = spread[0, :, at], spread[1, :, at]
        out_r = mr * total_r - mi * total_i
        out_i = mr * total_i + mi * total_r
        terms = inc_r * out_r + inc_i * out_i
        terms = jnp.sum(terms.reshape(modes // 8, 8, width), 0)
        part[...] += terms[:, :LANES] + terms[:, LANES:]
        even = (lax.broadcasted_iota(jnp.int32, (modes, LANES), 1) // dirs) % 2 == 0
        for p, out in ((0, out_r), (1, out_i)):
            left, right = out[:, :LANES], out[:, LANES:]
            head = jnp.where(even, left, right)
            tail = pltpu.roll(jnp.where(even, right, left), LANES - dirs, 1)
            rows = pl.ds(p * modes, modes)
            out_at[q, rows, :LANES] = head.astype(BF16)
            out_at[q, rows, LANES:] = tail.astype(BF16)
        pltpu.make_async_copy(out_at.at[q], scattered.at[:, at], stored.at[q]).start()
        return carry

    part[...] = jnp.zeros_like(part)
    lax.fori_loop(0, steps, step_body, 0)

    row = jnp.sum(part[...], 0, keepdims=True)
    part[...] = jnp.broadcast_to(row, part.shape)
    sends = []
    for r, peer in enumerate(everyone):
        copy = pltpu.make_async_remote_copy(
            src_ref=part, dst_ref=inbox.at[me], send_sem=ext_send.at[r], recv_sem=ext_recv.at[r],
            device_id={"sph": peer}, device_id_type=MESH,
        )
        copy.start()
        sends.append(copy)
    inbox[me] = part[...]
    for copy in copies:
        copy.wait_send()
    for q in range(steps):
        at = pl.ds(q * width, width)
        pltpu.make_async_copy(out_at.at[q], scattered.at[:, at], stored.at[q]).wait()
    for copy in sends:
        copy.wait_recv()
    row = jnp.sum(inbox[...], 0)[:1]
    shift = LANES // 2
    while shift >= dirs:
        row = row + pltpu.roll(row, shift, 1)
        shift //= 2
    ext[...] = row
    for copy in sends:
        copy.wait_send()


def shards(
    positions, wave_vectors, pattern, dir_index, mie, trans_table, pair_route, pair_source,
    pair_target, pair_class,
):
    modes = pattern.shape[1]
    spheres = positions.shape[0]
    dirs = dir_index.shape[0]
    blocks = spheres // BLOCK
    classes = trans_table.shape[0]
    devices = lax.axis_size("sph")
    pair_count = pair_source.shape[0]
    capacity = max(2, 2 * pair_count // devices)
    slots = devices * capacity
    chips = devices // 2
    bits = chips.bit_length() - 1
    per = LANES // dirs
    steps = blocks // per
    width = BLOCK * LANES
    depth = classes * modes
    columns = steps * width
    assert chips == 1 << bits and slots == LANES and per == len(ORDER[0]) and BLOCK == len(ORDER)

    vmem = pl.BlockSpec(memory_space=pltpu.VMEM)
    smem = pl.BlockSpec(memory_space=pltpu.SMEM)
    anywhere = pl.BlockSpec(memory_space=pl.ANY)
    dims = (modes, dirs, spheres, blocks, classes, devices, capacity)
    dma = pltpu.SemaphoreType.DMA
    scattered, ext = pl.pallas_call(
        functools.partial(fused_kernel, dims),
        out_shape=[
            jax.ShapeDtypeStruct((2 * modes, columns), BF16),
            jax.ShapeDtypeStruct((1, LANES), F32),
        ],
        in_specs=[vmem] * 4 + [smem, vmem, smem, smem, vmem, anywhere, anywhere],
        out_specs=[anywhere, vmem],
        scratch_shapes=[
            pltpu.VMEM(trans_table.shape, BF16),
            pltpu.VMEM(pattern.shape, F32),
            pltpu.VMEM((modes, depth), BF16),
            pltpu.VMEM((modes, depth), BF16),
            pltpu.VMEM((modes, depth), BF16),
            pltpu.VMEM((devices, spheres, 2 * modes), BF16),
            pltpu.VMEM((devices, 8, LANES), F32),
            pltpu.VMEM((BLOCK, 2 * modes, 2 * slots), BF16),
            pltpu.VMEM((depth, width), BF16),
            pltpu.VMEM((depth, width), BF16),
            pltpu.VMEM((depth, width), BF16),
            pltpu.VMEM((2, modes, LANES), F32),
            pltpu.VMEM((2, modes, columns), F32),
            pltpu.VMEM((2, modes, columns), F32),
            pltpu.VMEM((2, steps * BLOCK, LANES), F32),
            pltpu.VMEM((BLOCK, 2 * slots, LANES), F32),
            pltpu.VMEM((BLOCK, slots, LANES), jnp.int32),
            pltpu.VMEM((2 * modes, width), F32),
            pltpu.VMEM((steps, 2 * modes, width), BF16),
            pltpu.VMEM((8, LANES), F32),
            pltpu.VMEM((devices, 8, LANES), F32),
            dma((2,)),
            dma((steps,)),
            dma((2, chips * (bits + 1))),
            dma((2, 2 * chips)),
            dma((devices,)),
            dma((devices,)),
        ],
        compiler_params=pltpu.CompilerParams(
            collective_id=0, has_side_effects=True, vmem_limit_bytes=63 * 1024 * 1024
        ),
        name="fused",
    )(
        pair_route.reshape(1, pair_count), pair_source.reshape(1, pair_count),
        pair_target.reshape(1, pair_count), pair_class.reshape(1, pair_count),
        positions.T, positions.T, wave_vectors.T, dir_index, jnp.transpose(mie, (0, 2, 1)),
        pattern, trans_table,
    )
    return scattered, ext[0, :dirs]


def solution(mesh):
    placed = (
        P("sph", None), P(), P(), P("groups"), P(None, None, "sph"), P(),
        P("sph", None), P("sph"), P("sph"), P("sph"),
    )
    return jax.shard_map(
        shards,
        mesh=mesh,
        in_specs=placed,
        out_specs=(P(None, ("groups", "sph")), P("groups")),
        check_vma=False,
    )
```

```python
import functools

import jax
import jax.numpy as jnp
from jax import lax
from jax.experimental import pallas as pl
from jax.experimental.pallas import tpu as pltpu
from jax.sharding import PartitionSpec as P

BLOCK = 2
LANES = 128
HIGHEST = lax.Precision.HIGHEST
MESH = pl.DeviceIdType.MESH
F32 = jnp.float32
BF16 = jnp.bfloat16
ORDER = ((0, 2, 1, 3), (3, 0, 2, 1))
PARTS = 4
DEPTH = 512


def sincos(angle):
    turns = jnp.floor(angle * 0.6366197723675814 + 0.5)
    rest = angle - turns * 1.5703125
    rest = rest - turns * 4.837512969970703125e-4
    rest = rest - turns * 7.54978995489188216e-8
    square = rest * rest
    sine = rest + rest * square * (
        -1.6666654611e-1 + square * (8.3321608736e-3 + square * -1.9515295891e-4)
    )
    cosine = 1.0 - 0.5 * square + square * square * (
        4.166664568298827e-2 + square * (-1.388731625493765e-3 + square * 2.443315711809948e-5)
    )
    quarter = turns.astype(jnp.int32)
    swap = (quarter & 1) == 1
    c = jnp.where(swap, sine, cosine)
    s = jnp.where(swap, cosine, sine)
    c = jnp.where(((quarter + 1) & 2) == 2, -c, c)
    s = jnp.where((quarter & 2) == 2, -s, s)
    return c, s


def split_two(x):
    high = x.astype(BF16)
    return high, (x - high.astype(F32)).astype(BF16)


def fused_kernel(
    dims, route, source, target, kind, pos_s, pos_v, wave_s, dir_s, mie, pattern_hbm, table_hbm,
    scattered, ext,
    table, pattern, t_real, t_diff, t_sum, all_mie, all_small, weights, x_real, x_imag, x_sum,
    pat, inc, spread, own_e, phase, delta, out_at, part, inbox,
    loaded, stored, send, recv, ext_send, ext_recv,
):
    modes, dirs, spheres, blocks, classes, devices, capacity = dims
    chunk = modes // PARTS
    me = lax.axis_index("sph")
    chips = devices // 2
    chip, core = me // 2, me % 2
    other = chip * 2 + (1 - core)
    bits = []
    bit = chips // 2
    while bit >= 1:
        bits.append(bit)
        bit //= 2

    def flip(value, bit):
        return value + bit - 2 * bit * ((value // bit) % 2)

    partners = [flip(chip, bit) * 2 + core for bit in bits] + [other]
    everyone = [(me + r) % devices for r in range(1, devices)]

    barrier = pltpu.get_barrier_semaphore()
    for peer in partners:
        pl.semaphore_signal(barrier, inc=1, device_id={"sph": peer}, device_id_type=MESH)
    load_table = pltpu.make_async_copy(table_hbm, table, loaded.at[0])
    load_pattern = pltpu.make_async_copy(pattern_hbm, pattern, loaded.at[1])
    load_table.start()
    load_pattern.start()

    pairs = route.shape[1]
    slots = devices * capacity
    ia = lax.broadcasted_iota(jnp.int32, (pairs, pairs), 0)
    ib = lax.broadcasted_iota(jnp.int32, (pairs, pairs), 1)

    def column(row):
        return jnp.sum(jnp.where(ia == ib, row, 0.0), 1, keepdims=True)

    dest = route[...].astype(F32)
    dest_col = column(dest)
    rank = jnp.sum(jnp.where((dest_col == dest) & (ib < ia), 1.0, 0.0), 1, keepdims=True)
    slot_lane = lax.broadcasted_iota(jnp.int32, (pairs, LANES), 1).astype(F32)
    match = (dest_col * capacity + rank) == slot_lane
    source_col = column(source[...].astype(F32))
    cell_col = column((kind[...] * blocks + target[...] + 1).astype(F32))
    sphere_lane = lax.broadcasted_iota(jnp.int32, (pairs, spheres), 1).astype(F32)
    entries = [cell_col, source_col]
    for j in range(BLOCK):
        picked = sphere_lane == source_col * BLOCK + j
        for axis in range(3):
            entries.append(
                jnp.sum(jnp.where(picked, pos_v[axis : axis + 1, :], 0.0), 1, keepdims=True)
            )
    rows = [jnp.sum(jnp.where(match, entry, 0.0), 0, keepdims=True) for entry in entries]
    all_small[me] = jnp.concatenate(rows, 0)
    all_mie[me] = jnp.concatenate([mie[0], mie[1]], 1).astype(BF16)

    pl.semaphore_wait(barrier, len(partners))

    copies = []

    def start(origin, mask, step):
        slot = mask if step == len(bits) else mask + bits[step]
        slot = slot + chips if step == len(bits) else slot
        back = chips * step + mask
        for at, ref in ((0, all_small), (1, all_mie)):
            copy = pltpu.make_async_remote_copy(
                src_ref=ref.at[origin], dst_ref=ref.at[origin],
                send_sem=send.at[at, back], recv_sem=recv.at[at, slot],
                device_id={"sph": partners[step]}, device_id_type=MESH,
            )
            copy.start()
            copies.append(copy)

    def arrived(at, slot):
        ref = (all_small, all_mie)[at]
        pltpu.make_async_remote_copy(
            src_ref=ref.at[me], dst_ref=ref.at[me],
            send_sem=send.at[at, 0], recv_sem=recv.at[at, slot],
            device_id={"sph": other}, device_id_type=MESH,
        ).wait_recv()

    def low(mask):
        return mask & -mask

    def origin_of(mask):
        value = chip
        for bit in bits:
            if mask & bit:
                value = flip(value, bit)
        return value * 2 + core

    for step in range(len(bits) + 1):
        start(me, 0, step)

    def forward(mask):
        arrived(0, mask)
        arrived(1, mask)
        for step, bit in enumerate(bits):
            if bit < low(mask):
                start(origin_of(mask), mask, step)
        start(origin_of(mask), mask, len(bits))

    waits = sorted(range(1, chips), key=lambda mask: (bin(mask).count("1"), -mask))

    per = LANES // dirs
    lane = lax.broadcasted_iota(jnp.int32, (1, LANES), 1)
    group = lane // dirs
    k_rows = []
    dir_row = jnp.zeros((1, LANES), jnp.int32)
    for axis in range(3):
        k_rows.append(jnp.zeros((1, LANES), F32))
    for d in range(dirs):
        here = lane % dirs == d
        index = dir_s[d]
        dir_row = jnp.where(here, index, dir_row)
        for axis in range(3):
            k_rows[axis] = jnp.where(here, wave_s[axis, index], k_rows[axis])

    def block_of(j):
        order = jnp.zeros((1, LANES), jnp.int32)
        for g in range(per):
            order = jnp.where(group == g, ORDER[j][g], order)
        return order

    orders = [block_of(j) for j in range(BLOCK)]
    steps = blocks // per
    tiles = [(q, j) for q in range(steps) for j in range(BLOCK)]
    sphere_at = jnp.concatenate([(orders[j] + q * per) * BLOCK + j for q, j in tiles], 0)
    here = [jnp.zeros((len(tiles), LANES), F32) for _ in range(3)]
    for s in range(spheres):
        mine = sphere_at == s
        for axis in range(3):
            here[axis] = jnp.where(mine, pos_s[axis, s], here[axis])

    def phase_of(x, y, z):
        return sincos(x * k_rows[0] + y * k_rows[1] + z * k_rows[2])

    own_c, own_s = phase_of(*here)
    own_e[0] = own_c
    own_e[1] = own_s

    def prepare_table():
        load_table.wait()
        for c in range(0, classes, 2):
            at = pl.ds(c * modes, 2 * modes)
            real = jnp.concatenate([table[c, 0], table[c + 1, 0]], 1)
            imag = jnp.concatenate([table[c, 1], table[c + 1, 1]], 1)
            t_real[:, at] = real
            t_diff[:, at] = imag - real
            t_sum[:, at] = imag + real

    def prepare_field():
        load_pattern.wait()
        tables = pattern.shape[2]
        chosen = (lax.broadcasted_iota(jnp.int32, (tables, LANES), 0) == dir_row).astype(F32).astype(BF16)
        for p in range(2):
            high, rest = split_two(pattern[p])
            pat[p] = jnp.dot(high, chosen, preferred_element_type=F32) + jnp.dot(
                rest, chosen, preferred_element_type=F32
            )
        sphere_id = lax.broadcasted_iota(jnp.int32, (spheres, LANES), 0)
        picks = jnp.concatenate(
            [(sphere_id == sphere_at[t : t + 1]).astype(F32) for t in range(len(tiles))], 1
        )
        picks = jnp.concatenate([picks, picks], 0).astype(BF16)
        for p in range(2):
            pieces = jnp.concatenate(split_two(mie[p]), 0)
            spread[p] = lax.dot_general(
                pieces, picks, (((0,), (0,)), ((), ())), preferred_element_type=F32
            )
        for t in range(len(tiles)):
            at = pl.ds(t * LANES, LANES)
            c, s = own_c[t : t + 1], own_s[t : t + 1]
            inc[0, :, at] = c * pat[0] - s * pat[1]
            inc[1, :, at] = c * pat[1] + s * pat[0]

    for mask in waits[:1]:
        forward(mask)
    prepare_table()
    for mask in waits[1:3]:
        forward(mask)
    prepare_field()
    for mask in waits[3:]:
        forward(mask)
    for slot in range(chips):
        arrived(0, chips + slot)

    slot_id = lax.broadcasted_iota(jnp.int32, (slots, devices), 0)
    from_device = (slot_id // capacity == lax.broadcasted_iota(jnp.int32, (slots, devices), 1)).astype(F32)
    lists = jnp.concatenate([all_small[:, r, :] for r in range(8)], 1)
    lists = jnp.dot(from_device, lists, precision=HIGHEST, preferred_element_type=F32)
    slot_row = lax.broadcasted_iota(jnp.int32, (slots, LANES), 0)
    slot_lane = lax.broadcasted_iota(jnp.int32, (slots, LANES), 1)
    wanted = slot_lane == me * capacity + slot_row % capacity
    cols = [
        jnp.sum(jnp.where(wanted, lists[:, r * LANES : (r + 1) * LANES], 0.0), 1, keepdims=True)
        for r in range(8)
    ]
    cell = cols[0].astype(jnp.int32) - 1
    owner = lax.broadcasted_iota(jnp.int32, (slots, 1), 0) // capacity
    row_of = owner * spheres + cols[1].astype(jnp.int32) * BLOCK
    for j in range(BLOCK):
        c, s = phase_of(*cols[2 + 3 * j : 5 + 3 * j])
        phase[j, :slots, :] = c
        phase[j, slots:, :] = s
        delta[j] = cell - orders[j]
    total = devices * spheres
    at_row = lax.broadcasted_iota(jnp.int32, (slots, total), 1)
    pick = jnp.concatenate(
        [(at_row == row_of + j).astype(F32).astype(BF16) for j in range(BLOCK)], 0
    )

    for slot in range(chips):
        arrived(1, chips + slot)
    gathered = jnp.dot(
        pick, all_mie[...].reshape(total, 2 * modes), preferred_element_type=F32
    )
    for j in range(BLOCK):
        turned = gathered[j * slots : (j + 1) * slots].T.astype(BF16)
        real, imag = turned[:modes], turned[modes:]
        for g in range(PARTS):
            piece = slice(g * chunk, (g + 1) * chunk)
            upper = pl.ds(2 * g * chunk, chunk)
            lower = pl.ds((2 * g + 1) * chunk, chunk)
            weights[j, upper, :slots] = real[piece]
            weights[j, upper, slots:] = -imag[piece]
            weights[j, lower, :slots] = imag[piece]
            weights[j, lower, slots:] = real[piece]

    width = BLOCK * LANES

    def build(q):
        work = []
        for j in range(BLOCK):
            c_all, s_all = phase[j, :slots, :], phase[j, slots:, :]
            for c in range(0, classes, 2):
                tops, bottoms = [], []
                for h in range(2):
                    here = delta[j] == (c + h) * blocks + q * per
                    tops.append(jnp.where(here, c_all, 0.0))
                    bottoms.append(jnp.where(here, s_all, 0.0))
                masked = jnp.concatenate(
                    [jnp.concatenate(tops, 1), jnp.concatenate(bottoms, 1)], 0
                ).astype(BF16)
                for g in range(PARTS):
                    work.append(functools.partial(piece_of, q, j, c, g, masked))
        return work

    def piece_of(q, j, c, g, masked):
        both = pl.ds(2 * g * chunk, 2 * chunk)
        y = jnp.dot(weights[j, both, :], masked, preferred_element_type=F32)
        own = pl.ds(g * chunk, chunk)
        pr, pi = pat[0, own, :], pat[1, own, :]
        for h in range(2):
            at = slice(h * LANES, (h + 1) * LANES)
            yr, yi = y[:chunk, at], y[chunk:, at]
            mr = yr * pr - yi * pi
            mi = yr * pi + yi * pr
            rows = pl.ds((c + h) * modes + g * chunk, chunk)
            lanes = pl.ds(j * LANES, LANES)
            x_real[q, rows, lanes] = mr.astype(BF16)
            x_imag[q, rows, lanes] = mi.astype(BF16)
            x_sum[q, rows, lanes] = (mr + mi).astype(BF16)

    def finish(q, both, first, second):
        at = pl.ds(q * width, width)
        inc_r, inc_i = inc[0, :, at], inc[1, :, at]
        total_r = inc_r + (both - second)
        total_i = inc_i + (both + first)
        mr, mi = spread[0, :, at], spread[1, :, at]
        out_r = mr * total_r - mi * total_i
        out_i = mr * total_i + mi * total_r
        terms = inc_r * out_r + inc_i * out_i
        terms = jnp.sum(terms.reshape(modes // 8, 8, width), 0)
        part[...] += terms[:, :LANES] + terms[:, LANES:]
        even = (lax.broadcasted_iota(jnp.int32, (modes, LANES), 1) // dirs) % 2 == 0
        for p, out in ((0, out_r), (1, out_i)):
            left, right = out[:, :LANES], out[:, LANES:]
            head = jnp.where(even, left, right)
            tail = pltpu.roll(jnp.where(even, right, left), LANES - dirs, 1)
            rows = pl.ds(p * modes, modes)
            out_at[q, rows, :LANES] = head.astype(BF16)
            out_at[q, rows, LANES:] = tail.astype(BF16)

    part[...] = jnp.zeros_like(part)
    for work in build(0):
        work()
    pairs_of = ((t_real, x_sum), (t_diff, x_real), (t_sum, x_imag))
    deep = classes * modes // DEPTH
    for q in range(steps):
        todo = build(q + 1) if q + 1 < steps else []
        done = 0
        results = []
        for n, (matrix, mixed) in enumerate(pairs_of):
            value = None
            for i in range(deep):
                at = slice(i * DEPTH, (i + 1) * DEPTH)
                term = jnp.dot(matrix[:, at], mixed[q, at, :], preferred_element_type=F32)
                value = term if value is None else value + term
                while done < (n * deep + i + 1) * len(todo) // (3 * deep):
                    todo[done]()
                    done += 1
            results.append(value)
        finish(q, *results)

    for q in range(steps):
        at = pl.ds(q * width, width)
        pltpu.make_async_copy(out_at.at[q], scattered.at[:, at], stored.at[q]).start()
    row = jnp.sum(part[...], 0, keepdims=True)
    part[0:1, :] = row
    sends = []
    for r, peer in enumerate(everyone):
        copy = pltpu.make_async_remote_copy(
            src_ref=part.at[pl.ds(0, 1)], dst_ref=inbox.at[me], send_sem=ext_send.at[r], recv_sem=ext_recv.at[r],
            device_id={"sph": peer}, device_id_type=MESH,
        )
        copy.start()
        sends.append(copy)
    inbox[me] = row
    for copy in copies:
        copy.wait_send()
    for q in range(steps):
        at = pl.ds(q * width, width)
        pltpu.make_async_copy(out_at.at[q], scattered.at[:, at], stored.at[q]).wait()
    for copy in sends:
        copy.wait_recv()
    row = jnp.sum(inbox[...], 0)
    shift = LANES // 2
    while shift >= dirs:
        row = row + pltpu.roll(row, shift, 1)
        shift //= 2
    ext[...] = row
    for copy in sends:
        copy.wait_send()


def shards(
    positions, wave_vectors, pattern, dir_index, mie, trans_table, pair_route, pair_source,
    pair_target, pair_class,
):
    modes = pattern.shape[1]
    spheres = positions.shape[0]
    dirs = dir_index.shape[0]
    blocks = spheres // BLOCK
    classes = trans_table.shape[0]
    devices = lax.axis_size("sph")
    pair_count = pair_source.shape[0]
    capacity = max(2, 2 * pair_count // devices)
    slots = devices * capacity
    chips = devices // 2
    bits = chips.bit_length() - 1
    per = LANES // dirs
    steps = blocks // per
    width = BLOCK * LANES
    depth = classes * modes
    columns = steps * width
    assert modes % (16 * PARTS) == 0 and depth % DEPTH == 0 and classes % 2 == 0
    assert chips == 1 << bits and slots == LANES and per == len(ORDER[0]) and BLOCK == len(ORDER)

    vmem = pl.BlockSpec(memory_space=pltpu.VMEM)
    smem = pl.BlockSpec(memory_space=pltpu.SMEM)
    anywhere = pl.BlockSpec(memory_space=pl.ANY)
    dims = (modes, dirs, spheres, blocks, classes, devices, capacity)
    dma = pltpu.SemaphoreType.DMA
    scattered, ext = pl.pallas_call(
        functools.partial(fused_kernel, dims),
        out_shape=[
            jax.ShapeDtypeStruct((2 * modes, columns), BF16),
            jax.ShapeDtypeStruct((1, LANES), F32),
        ],
        in_specs=[vmem] * 4 + [smem, vmem, smem, smem, vmem, anywhere, anywhere],
        out_specs=[anywhere, vmem],
        scratch_shapes=[
            pltpu.VMEM(trans_table.shape, BF16),
            pltpu.VMEM(pattern.shape, F32),
            pltpu.VMEM((modes, depth), BF16),
            pltpu.VMEM((modes, depth), BF16),
            pltpu.VMEM((modes, depth), BF16),
            pltpu.VMEM((devices, spheres, 2 * modes), BF16),
            pltpu.VMEM((devices, 8, LANES), F32),
            pltpu.VMEM((BLOCK, 2 * modes, 2 * slots), BF16),
            pltpu.VMEM((steps, depth, width), BF16),
            pltpu.VMEM((steps, depth, width), BF16),
            pltpu.VMEM((steps, depth, width), BF16),
            pltpu.VMEM((2, modes, LANES), F32),
            pltpu.VMEM((2, modes, columns), F32),
            pltpu.VMEM((2, modes, columns), F32),
            pltpu.VMEM((2, steps * BLOCK, LANES), F32),
            pltpu.VMEM((BLOCK, 2 * slots, LANES), F32),
            pltpu.VMEM((BLOCK, slots, LANES), jnp.int32),
            pltpu.VMEM((steps, 2 * modes, width), BF16),
            pltpu.VMEM((8, LANES), F32),
            pltpu.VMEM((devices, 1, LANES), F32),
            dma((2,)),
            dma((steps,)),
            dma((2, chips * (bits + 1))),
            dma((2, 2 * chips)),
            dma((devices,)),
            dma((devices,)),
        ],
        compiler_params=pltpu.CompilerParams(
            collective_id=0, has_side_effects=True, vmem_limit_bytes=63 * 1024 * 1024
        ),
        name="fused",
    )(
        pair_route.reshape(1, pair_count), pair_source.reshape(1, pair_count),
        pair_target.reshape(1, pair_count), pair_class.reshape(1, pair_count),
        positions.T, positions.T, wave_vectors.T, dir_index, jnp.transpose(mie, (0, 2, 1)),
        pattern, trans_table,
    )
    return scattered, ext[0, :dirs]


def solution(mesh):
    placed = (
        P("sph", None), P(), P(), P("groups"), P(None, None, "sph"), P(),
        P("sph", None), P("sph"), P("sph"), P("sph"),
    )
    return jax.shard_map(
        shards,
        mesh=mesh,
        in_specs=placed,
        out_specs=(P(None, ("groups", "sph")), P("groups")),
        check_vma=False,
    )
```

```python
import functools

import jax
import jax.numpy as jnp
from jax import lax
from jax.experimental import pallas as pl
from jax.experimental.pallas import tpu as pltpu
from jax.sharding import PartitionSpec as P

BLOCK = 2
LANES = 128
HIGHEST = lax.Precision.HIGHEST
MESH = pl.DeviceIdType.MESH
F32 = jnp.float32
BF16 = jnp.bfloat16
ORDER = ((0, 2, 1, 3), (3, 0, 2, 1))
PARTS = 4
DEPTH = 512


def sincos(angle):
    turns = jnp.floor(angle * 0.6366197723675814 + 0.5)
    rest = angle - turns * 1.5703125
    rest = rest - turns * 4.837512969970703125e-4
    rest = rest - turns * 7.54978995489188216e-8
    square = rest * rest
    sine = rest + rest * square * (
        -1.6666654611e-1 + square * (8.3321608736e-3 + square * -1.9515295891e-4)
    )
    cosine = 1.0 - 0.5 * square + square * square * (
        4.166664568298827e-2 + square * (-1.388731625493765e-3 + square * 2.443315711809948e-5)
    )
    quarter = turns.astype(jnp.int32)
    swap = (quarter & 1) == 1
    c = jnp.where(swap, sine, cosine)
    s = jnp.where(swap, cosine, sine)
    c = jnp.where(((quarter + 1) & 2) == 2, -c, c)
    s = jnp.where((quarter & 2) == 2, -s, s)
    return c, s


def split_two(x):
    high = x.astype(BF16)
    return high, (x - high.astype(F32)).astype(BF16)


def fused_kernel(
    dims, route_hbm, source_hbm, target_hbm, kind_hbm, pos_hbm, wave_hbm, dir_hbm, mie_hbm,
    pattern_hbm, table_hbm, scattered, ext,
    route, source, target, kind, pos_s, pos_v, wave_s, dir_s, mie, table, pattern, t_real, t_diff, t_sum, all_mie, all_small, weights, x_real, x_imag, x_sum,
    pat, inc, spread, own_e, phase, delta, part, inbox,
    loaded, send, recv, ext_send, ext_recv,
):
    modes, dirs, spheres, blocks, classes, devices, capacity = dims
    chunk = modes // PARTS
    me = lax.axis_index("sph")
    chips = devices // 2
    chip, core = me // 2, me % 2
    other = chip * 2 + (1 - core)
    bits = []
    bit = chips // 2
    while bit >= 1:
        bits.append(bit)
        bit //= 2

    def flip(value, bit):
        return value + bit - 2 * bit * ((value // bit) % 2)

    def chip_at(mask):
        value = chip
        for bit in bits:
            if mask & bit:
                value = flip(value, bit)
        return value

    stages = [[bit] for bit in bits[:-2]] + [bits[-2:] + [sum(bits[-2:])] if len(bits) > 1 else bits]
    held, routes = [0], []
    for stage, offsets in enumerate(stages):
        routes.append((list(held), offsets))
        held = held + [h | o for o in offsets for h in held]
    stage_of = {0: -1}
    for stage, (before, offsets) in enumerate(routes):
        for o in offsets:
            for h in before:
                stage_of[h | o] = stage
    greeted = [o for offsets in stages for o in offsets]
    partners = [chip_at(o) * 2 + core for o in greeted] + [other]
    everyone = [(me + r) % devices for r in range(1, devices)]

    barrier = pltpu.get_barrier_semaphore()
    for peer in partners:
        pl.semaphore_signal(barrier, inc=1, device_id={"sph": peer}, device_id_type=MESH)
    load_table = pltpu.make_async_copy(table_hbm, table, loaded.at[0])
    load_pattern = pltpu.make_async_copy(pattern_hbm, pattern, loaded.at[1])
    small = (
        (route_hbm, route), (source_hbm, source), (target_hbm, target), (kind_hbm, kind),
        (pos_hbm, pos_v), (mie_hbm, mie), (pos_hbm, pos_s), (wave_hbm, wave_s), (dir_hbm, dir_s),
    )
    fetches = [pltpu.make_async_copy(a, b, loaded.at[2 + i]) for i, (a, b) in enumerate(small)]
    for copy in fetches:
        copy.start()
    load_pattern.start()
    load_table.start()
    for copy in fetches:
        copy.wait()

    pairs = route.shape[1]
    slots = devices * capacity
    ia = lax.broadcasted_iota(jnp.int32, (pairs, pairs), 0)
    ib = lax.broadcasted_iota(jnp.int32, (pairs, pairs), 1)

    def column(row):
        return jnp.sum(jnp.where(ia == ib, row, 0.0), 1, keepdims=True)

    dest = route[...].astype(F32)
    dest_col = column(dest)
    rank = jnp.sum(jnp.where((dest_col == dest) & (ib < ia), 1.0, 0.0), 1, keepdims=True)
    slot_lane = lax.broadcasted_iota(jnp.int32, (pairs, LANES), 1).astype(F32)
    match = (dest_col * capacity + rank) == slot_lane
    source_col = column(source[...].astype(F32))
    cell_col = column((kind[...] * blocks + target[...] + 1).astype(F32))
    sphere_lane = lax.broadcasted_iota(jnp.int32, (pairs, spheres), 1).astype(F32)
    entries = [cell_col, source_col]
    for j in range(BLOCK):
        picked = sphere_lane == source_col * BLOCK + j
        for axis in range(3):
            entries.append(
                jnp.sum(jnp.where(picked, pos_v[axis : axis + 1, :], 0.0), 1, keepdims=True)
            )
    rows = [jnp.sum(jnp.where(match, entry, 0.0), 0, keepdims=True) for entry in entries]
    all_small[me] = jnp.concatenate(rows, 0)
    all_mie[me] = jnp.concatenate([mie[0], mie[1]], 1).astype(BF16)

    pl.semaphore_wait(barrier, len(partners))

    copies = []
    items = (all_small, all_mie)

    def start(at, mask, offset):
        ref = items[at].at[chip_at(mask) * 2 + core]
        slot = chips + mask if offset is None else mask | offset
        target = other if offset is None else chip_at(offset) * 2 + core
        copy = pltpu.make_async_remote_copy(
            src_ref=ref, dst_ref=ref, send_sem=send.at[at, len(copies) // 2],
            recv_sem=recv.at[at, slot], device_id={"sph": target}, device_id_type=MESH,
        )
        copy.start()
        copies.append(copy)

    def arrived(at, slot):
        ref = items[at].at[me]
        pltpu.make_async_remote_copy(
            src_ref=ref, dst_ref=ref, send_sem=send.at[at, 0], recv_sem=recv.at[at, slot],
            device_id={"sph": other}, device_id_type=MESH,
        ).wait_recv()

    def hand_on(mask):
        later = [o for offsets in stages[stage_of[mask] + 1 :] for o in offsets]
        for offset in later + [None]:
            for at in range(2):
                start(at, mask, offset)

    def forward(mask):
        for at in range(2):
            arrived(at, mask)
        hand_on(mask)

    hand_on(0)
    waits = sorted(range(1, chips), key=lambda m: (bin(m).count("1"), -m))

    per = LANES // dirs
    lane = lax.broadcasted_iota(jnp.int32, (1, LANES), 1)
    group = lane // dirs
    k_rows = []
    dir_row = jnp.zeros((1, LANES), jnp.int32)
    for axis in range(3):
        k_rows.append(jnp.zeros((1, LANES), F32))
    for d in range(dirs):
        here = lane % dirs == d
        index = dir_s[d]
        dir_row = jnp.where(here, index, dir_row)
        for axis in range(3):
            k_rows[axis] = jnp.where(here, wave_s[axis, index], k_rows[axis])

    def block_of(j):
        order = jnp.zeros((1, LANES), jnp.int32)
        for g in range(per):
            order = jnp.where(group == g, ORDER[j][g], order)
        return order

    orders = [block_of(j) for j in range(BLOCK)]
    steps = blocks // per
    tiles = [(q, j) for q in range(steps) for j in range(BLOCK)]
    sphere_at = jnp.concatenate([(orders[j] + q * per) * BLOCK + j for q, j in tiles], 0)
    here = [jnp.zeros((len(tiles), LANES), F32) for _ in range(3)]
    for s in range(spheres):
        mine = sphere_at == s
        for axis in range(3):
            here[axis] = jnp.where(mine, pos_s[axis, s], here[axis])

    def phase_of(x, y, z):
        return sincos(x * k_rows[0] + y * k_rows[1] + z * k_rows[2])

    own_c, own_s = phase_of(*here)
    own_e[0] = own_c
    own_e[1] = own_s

    def prepare_table():
        load_table.wait()
        for c in range(0, classes, 2):
            at = pl.ds(c * modes, 2 * modes)
            real = jnp.concatenate([table[c, 0], table[c + 1, 0]], 1)
            imag = jnp.concatenate([table[c, 1], table[c + 1, 1]], 1)
            t_real[:, at] = real
            t_diff[:, at] = imag - real
            t_sum[:, at] = imag + real

    def prepare_field():
        load_pattern.wait()
        tables = pattern.shape[2]
        chosen = (lax.broadcasted_iota(jnp.int32, (tables, LANES), 0) == dir_row).astype(F32).astype(BF16)
        for p in range(2):
            high, rest = split_two(pattern[p])
            pat[p] = jnp.dot(high, chosen, preferred_element_type=F32) + jnp.dot(
                rest, chosen, preferred_element_type=F32
            )
        sphere_id = lax.broadcasted_iota(jnp.int32, (spheres, LANES), 0)
        picks = jnp.concatenate(
            [(sphere_id == sphere_at[t : t + 1]).astype(F32) for t in range(len(tiles))], 1
        )
        picks = jnp.concatenate([picks, picks], 0).astype(BF16)
        for p in range(2):
            pieces = jnp.concatenate(split_two(mie[p]), 0)
            spread[p] = lax.dot_general(
                pieces, picks, (((0,), (0,)), ((), ())), preferred_element_type=F32
            )
        for t in range(len(tiles)):
            at = pl.ds(t * LANES, LANES)
            c, s = own_c[t : t + 1], own_s[t : t + 1]
            inc[0, :, at] = c * pat[0] - s * pat[1]
            inc[1, :, at] = c * pat[1] + s * pat[0]

    prepare_table()
    early = [m for m in waits if m in greeted][:3]
    for mask in early:
        forward(mask)
    prepare_field()
    for mask in waits:
        if mask not in early:
            forward(mask)
    for slot in range(chips):
        arrived(0, chips + slot)

    slot_id = lax.broadcasted_iota(jnp.int32, (slots, devices), 0)
    from_device = (slot_id // capacity == lax.broadcasted_iota(jnp.int32, (slots, devices), 1)).astype(F32)
    lists = jnp.concatenate([all_small[:, r, :] for r in range(8)], 1)
    lists = jnp.dot(from_device, lists, precision=HIGHEST, preferred_element_type=F32)
    slot_row = lax.broadcasted_iota(jnp.int32, (slots, LANES), 0)
    slot_lane = lax.broadcasted_iota(jnp.int32, (slots, LANES), 1)
    wanted = slot_lane == me * capacity + slot_row % capacity
    cols = [
        jnp.sum(jnp.where(wanted, lists[:, r * LANES : (r + 1) * LANES], 0.0), 1, keepdims=True)
        for r in range(8)
    ]
    cell = cols[0].astype(jnp.int32) - 1
    owner = lax.broadcasted_iota(jnp.int32, (slots, 1), 0) // capacity
    row_of = owner * spheres + cols[1].astype(jnp.int32) * BLOCK
    for j in range(BLOCK):
        c, s = phase_of(*cols[2 + 3 * j : 5 + 3 * j])
        phase[j, :slots, :] = c
        phase[j, slots:, :] = s
        delta[j] = cell - orders[j]
    total = devices * spheres
    at_row = lax.broadcasted_iota(jnp.int32, (slots, total), 1)
    pick = jnp.concatenate(
        [(at_row == row_of + j).astype(F32).astype(BF16) for j in range(BLOCK)], 0
    )

    for slot in range(chips):
        arrived(1, chips + slot)
    gathered = jnp.dot(
        pick, all_mie[...].reshape(total, 2 * modes), preferred_element_type=F32
    )
    for j in range(BLOCK):
        turned = gathered[j * slots : (j + 1) * slots].T.astype(BF16)
        real, imag = turned[:modes], turned[modes:]
        for g in range(PARTS):
            piece = slice(g * chunk, (g + 1) * chunk)
            upper = pl.ds(2 * g * chunk, chunk)
            lower = pl.ds((2 * g + 1) * chunk, chunk)
            weights[j, upper, :slots] = real[piece]
            weights[j, upper, slots:] = -imag[piece]
            weights[j, lower, :slots] = imag[piece]
            weights[j, lower, slots:] = real[piece]

    width = BLOCK * LANES

    def build(q):
        work = []
        for j in range(BLOCK):
            c_all, s_all = phase[j, :slots, :], phase[j, slots:, :]
            for c in range(0, classes, 2):
                tops, bottoms = [], []
                for h in range(2):
                    here = delta[j] == (c + h) * blocks + q * per
                    tops.append(jnp.where(here, c_all, 0.0))
                    bottoms.append(jnp.where(here, s_all, 0.0))
                masked = jnp.concatenate(
                    [jnp.concatenate(tops, 1), jnp.concatenate(bottoms, 1)], 0
                ).astype(BF16)
                for g in range(PARTS):
                    work.append(functools.partial(piece_of, q, j, c, g, masked))
        return work

    def piece_of(q, j, c, g, masked):
        both = pl.ds(2 * g * chunk, 2 * chunk)
        y = jnp.dot(weights[j, both, :], masked, preferred_element_type=F32)
        own = pl.ds(g * chunk, chunk)
        pr, pi = pat[0, own, :], pat[1, own, :]
        for h in range(2):
            at = slice(h * LANES, (h + 1) * LANES)
            yr, yi = y[:chunk, at], y[chunk:, at]
            mr = yr * pr - yi * pi
            mi = yr * pi + yi * pr
            rows = pl.ds((c + h) * modes + g * chunk, chunk)
            lanes = pl.ds(j * LANES, LANES)
            x_real[q % 2, rows, lanes] = mr.astype(BF16)
            x_imag[q % 2, rows, lanes] = mi.astype(BF16)
            x_sum[q % 2, rows, lanes] = (mr + mi).astype(BF16)

    def finish(q, both, first, second):
        at = pl.ds(q * width, width)
        inc_r, inc_i = inc[0, :, at], inc[1, :, at]
        total_r = inc_r + (both - second)
        total_i = inc_i + (both + first)
        mr, mi = spread[0, :, at], spread[1, :, at]
        out_r = mr * total_r - mi * total_i
        out_i = mr * total_i + mi * total_r
        terms = inc_r * out_r + inc_i * out_i
        terms = jnp.sum(terms.reshape(modes // 8, 8, width), 0)
        part[...] += terms[:, :LANES] + terms[:, LANES:]
        even = (lax.broadcasted_iota(jnp.int32, (modes, LANES), 1) // dirs) % 2 == 0
        for p, out in ((0, out_r), (1, out_i)):
            left, right = out[:, :LANES], out[:, LANES:]
            head = jnp.where(even, left, right)
            tail = pltpu.roll(jnp.where(even, right, left), LANES - dirs, 1)
            rows = pl.ds(p * modes, modes)
            scattered[rows, pl.ds(q * width, LANES)] = head.astype(BF16)
            scattered[rows, pl.ds(q * width + LANES, LANES)] = tail.astype(BF16)

    part[...] = jnp.zeros_like(part)
    for work in build(0):
        work()
    pairs_of = ((t_real, x_sum), (t_diff, x_real), (t_sum, x_imag))
    deep = classes * modes // DEPTH
    for q in range(steps):
        todo = build(q + 1) if q + 1 < steps else []
        done = 0
        results = []
        for n, (matrix, mixed) in enumerate(pairs_of):
            value = None
            for i in range(deep):
                at = slice(i * DEPTH, (i + 1) * DEPTH)
                term = jnp.dot(matrix[:, at], mixed[q % 2, at, :], preferred_element_type=F32)
                value = term if value is None else value + term
                while done < (n * deep + i + 1) * len(todo) // (3 * deep):
                    todo[done]()
                    done += 1
            results.append(value)
        finish(q, *results)

    row = jnp.sum(part[...], 0, keepdims=True)
    part[0:1, :] = row
    sends = []
    for r, peer in enumerate(everyone):
        copy = pltpu.make_async_remote_copy(
            src_ref=part.at[pl.ds(0, 1)], dst_ref=inbox.at[me], send_sem=ext_send.at[r], recv_sem=ext_recv.at[r],
            device_id={"sph": peer}, device_id_type=MESH,
        )
        copy.start()
        sends.append(copy)
    inbox[me] = row
    for copy in copies:
        copy.wait_send()
    for copy in sends:
        copy.wait_recv()
    row = jnp.sum(inbox[...], 0)
    shift = LANES // 2
    while shift >= dirs:
        row = row + pltpu.roll(row, shift, 1)
        shift //= 2
    ext[...] = row
    for copy in sends:
        copy.wait_send()


def shards(
    positions, wave_vectors, pattern, dir_index, mie, trans_table, pair_route, pair_source,
    pair_target, pair_class,
):
    modes = pattern.shape[1]
    spheres = positions.shape[0]
    dirs = dir_index.shape[0]
    blocks = spheres // BLOCK
    classes = trans_table.shape[0]
    devices = lax.axis_size("sph")
    pair_count = pair_source.shape[0]
    capacity = max(2, 2 * pair_count // devices)
    slots = devices * capacity
    chips = devices // 2
    bits = chips.bit_length() - 1
    per = LANES // dirs
    steps = blocks // per
    width = BLOCK * LANES
    depth = classes * modes
    columns = steps * width
    assert modes % (16 * PARTS) == 0 and depth % DEPTH == 0 and classes % 2 == 0
    assert chips == 1 << bits and slots == LANES and per == len(ORDER[0]) and BLOCK == len(ORDER)

    vmem = pl.BlockSpec(memory_space=pltpu.VMEM)
    dims = (modes, dirs, spheres, blocks, classes, devices, capacity)
    dma = pltpu.SemaphoreType.DMA
    scattered, ext = pl.pallas_call(
        functools.partial(fused_kernel, dims),
        out_shape=[
            jax.ShapeDtypeStruct((2 * modes, columns), BF16),
            jax.ShapeDtypeStruct((1, LANES), F32),
        ],
        in_specs=[pl.BlockSpec(memory_space=pltpu.HBM)] * 10,
        out_specs=[vmem, vmem],
        scratch_shapes=[
            pltpu.VMEM((1, pair_count), jnp.int32),
            pltpu.VMEM((1, pair_count), jnp.int32),
            pltpu.VMEM((1, pair_count), jnp.int32),
            pltpu.VMEM((1, pair_count), jnp.int32),
            pltpu.SMEM((3, spheres), F32),
            pltpu.VMEM((3, spheres), F32),
            pltpu.SMEM((3, wave_vectors.shape[0]), F32),
            pltpu.SMEM((dirs,), jnp.int32),
            pltpu.VMEM((2, spheres, modes), F32),
            pltpu.VMEM(trans_table.shape, BF16),
            pltpu.VMEM(pattern.shape, F32),
            pltpu.VMEM((modes, depth), BF16),
            pltpu.VMEM((modes, depth), BF16),
            pltpu.VMEM((modes, depth), BF16),
            pltpu.VMEM((devices, spheres, 2 * modes), BF16),
            pltpu.VMEM((devices, 8, LANES), F32),
            pltpu.VMEM((BLOCK, 2 * modes, 2 * slots), BF16),
            pltpu.VMEM((2, depth, width), BF16),
            pltpu.VMEM((2, depth, width), BF16),
            pltpu.VMEM((2, depth, width), BF16),
            pltpu.VMEM((2, modes, LANES), F32),
            pltpu.VMEM((2, modes, columns), F32),
            pltpu.VMEM((2, modes, columns), F32),
            pltpu.VMEM((2, steps * BLOCK, LANES), F32),
            pltpu.VMEM((BLOCK, 2 * slots, LANES), F32),
            pltpu.VMEM((BLOCK, slots, LANES), jnp.int32),
            pltpu.VMEM((8, LANES), F32),
            pltpu.VMEM((devices, 1, LANES), F32),
            dma((11,)),
            dma((2, 2 * chips)),
            dma((2, 2 * chips)),
            dma((devices,)),
            dma((devices,)),
        ],
        compiler_params=pltpu.CompilerParams(
            collective_id=0, has_side_effects=True, vmem_limit_bytes=48 * 1024 * 1024
        ),
        name="fused",
    )(
        *[pltpu.with_memory_space_constraint(x, pltpu.HBM) for x in (
        pair_route.reshape(1, pair_count), pair_source.reshape(1, pair_count),
        pair_target.reshape(1, pair_count), pair_class.reshape(1, pair_count),
        positions.T, wave_vectors.T, dir_index, jnp.transpose(mie, (0, 2, 1)),
        pattern, trans_table,
        )]
    )
    return scattered, ext[0, :dirs]


def solution(mesh):
    placed = (
        P("sph", None), P(), P(), P("groups"), P(None, None, "sph"), P(),
        P("sph", None), P("sph"), P("sph"), P("sph"),
    )
    return jax.shard_map(
        shards,
        mesh=mesh,
        in_specs=placed,
        out_specs=(P(None, ("groups", "sph")), P("groups")),
        check_vma=False,
    )
```

```python
import functools

import jax
import jax.numpy as jnp
from jax import lax
from jax.experimental import pallas as pl
from jax.experimental.pallas import tpu as pltpu
from jax.sharding import PartitionSpec as P

BLOCK = 2
LANES = 128
HIGHEST = lax.Precision.HIGHEST
MESH = pl.DeviceIdType.MESH
F32 = jnp.float32
BF16 = jnp.bfloat16
ORDER = ((0, 2, 1, 3), (3, 0, 2, 1))
PARTS = 4
DEPTH = 512
SPLIT = 2


def sincos(angle):
    turns = jnp.floor(angle * 0.6366197723675814 + 0.5)
    rest = angle - turns * 1.5703125
    rest = rest - turns * 4.837512969970703125e-4
    rest = rest - turns * 7.54978995489188216e-8
    square = rest * rest
    sine = rest + rest * square * (
        -1.6666654611e-1 + square * (8.3321608736e-3 + square * -1.9515295891e-4)
    )
    cosine = 1.0 - 0.5 * square + square * square * (
        4.166664568298827e-2 + square * (-1.388731625493765e-3 + square * 2.443315711809948e-5)
    )
    quarter = turns.astype(jnp.int32)
    swap = (quarter & 1) == 1
    c = jnp.where(swap, sine, cosine)
    s = jnp.where(swap, cosine, sine)
    c = jnp.where(((quarter + 1) & 2) == 2, -c, c)
    s = jnp.where((quarter & 2) == 2, -s, s)
    return c, s


def split_two(x):
    high = x.astype(BF16)
    return high, (x - high.astype(F32)).astype(BF16)


def fused_kernel(
    dims, route_hbm, source_hbm, target_hbm, kind_hbm, pos_hbm, wave_hbm, dir_hbm, mie_hbm,
    pattern_hbm, table_hbm, scattered, ext,
    route, source, target, kind, pos_s, pos_v, wave_s, dir_s, mie, table, pattern, t_real, t_diff, t_sum, all_mie, all_small, weights, x_real, x_imag, x_sum,
    pat, inc, spread, own_e, phase, delta, part, inbox,
    loaded, send, recv, ext_send, ext_recv,
):
    modes, dirs, spheres, blocks, classes, devices, capacity = dims
    chunk = modes // PARTS
    me = lax.axis_index("sph")
    chips = devices // 2
    chip, core = me // 2, me % 2
    other = chip * 2 + (1 - core)
    bits = []
    bit = chips // 2
    while bit >= 1:
        bits.append(bit)
        bit //= 2

    def flip(value, bit):
        return value + bit - 2 * bit * ((value // bit) % 2)

    def chip_at(mask):
        value = chip
        for bit in bits:
            if mask & bit:
                value = flip(value, bit)
        return value

    stages = [[bit] for bit in bits[:-2]] + [bits[-2:] + [sum(bits[-2:])] if len(bits) > 1 else bits]
    held, routes = [0], []
    for stage, offsets in enumerate(stages):
        routes.append((list(held), offsets))
        held = held + [h | o for o in offsets for h in held]
    stage_of = {0: -1}
    for stage, (before, offsets) in enumerate(routes):
        for o in offsets:
            for h in before:
                stage_of[h | o] = stage
    greeted = [o for offsets in stages for o in offsets]
    partners = [chip_at(o) * 2 + core for o in greeted] + [other]
    everyone = [(me + r) % devices for r in range(1, devices)]

    barrier = pltpu.get_barrier_semaphore()
    for peer in partners:
        pl.semaphore_signal(barrier, inc=1, device_id={"sph": peer}, device_id_type=MESH)
    load_table = pltpu.make_async_copy(table_hbm, table, loaded.at[0])
    load_pattern = pltpu.make_async_copy(pattern_hbm, pattern, loaded.at[1])
    small = (
        (route_hbm, route), (source_hbm, source), (target_hbm, target), (kind_hbm, kind),
        (pos_hbm, pos_v), (mie_hbm, mie), (pos_hbm, pos_s), (wave_hbm, wave_s), (dir_hbm, dir_s),
    )
    fetches = [pltpu.make_async_copy(a, b, loaded.at[2 + i]) for i, (a, b) in enumerate(small)]
    for copy in fetches:
        copy.start()
    load_pattern.start()
    load_table.start()
    for copy in fetches:
        copy.wait()

    pairs = route.shape[1]
    slots = devices * capacity
    ia = lax.broadcasted_iota(jnp.int32, (pairs, pairs), 0)
    ib = lax.broadcasted_iota(jnp.int32, (pairs, pairs), 1)

    def column(row):
        return jnp.sum(jnp.where(ia == ib, row, 0.0), 1, keepdims=True)

    dest = route[...].astype(F32)
    dest_col = column(dest)
    rank = jnp.sum(jnp.where((dest_col == dest) & (ib < ia), 1.0, 0.0), 1, keepdims=True)
    slot_lane = lax.broadcasted_iota(jnp.int32, (pairs, LANES), 1).astype(F32)
    match = (dest_col * capacity + rank) == slot_lane
    source_col = column(source[...].astype(F32))
    cell_col = column((kind[...] * blocks + target[...] + 1).astype(F32))
    sphere_lane = lax.broadcasted_iota(jnp.int32, (pairs, spheres), 1).astype(F32)
    entries = [cell_col, source_col]
    for j in range(BLOCK):
        picked = sphere_lane == source_col * BLOCK + j
        for axis in range(3):
            entries.append(
                jnp.sum(jnp.where(picked, pos_v[axis : axis + 1, :], 0.0), 1, keepdims=True)
            )
    rows = [jnp.sum(jnp.where(match, entry, 0.0), 0, keepdims=True) for entry in entries]
    all_small[me] = jnp.concatenate(rows, 0)
    all_mie[me] = jnp.concatenate([mie[0], mie[1]], 1).astype(BF16)

    pl.semaphore_wait(barrier, len(partners))

    copies = ([], [])
    items = (all_small, all_mie)

    def start(at, mask, offset):
        ref = items[at].at[chip_at(mask) * 2 + core]
        slot = chips + mask if offset is None else mask | offset
        target = other if offset is None else chip_at(offset) * 2 + core
        copy = pltpu.make_async_remote_copy(
            src_ref=ref, dst_ref=ref, send_sem=send.at[at, len(copies[at])],
            recv_sem=recv.at[at, slot], device_id={"sph": target}, device_id_type=MESH,
        )
        copy.start()
        copies[at].append(copy)

    def arrived(at, slot):
        ref = items[at].at[me]
        pltpu.make_async_remote_copy(
            src_ref=ref, dst_ref=ref, send_sem=send.at[at, 0], recv_sem=recv.at[at, slot],
            device_id={"sph": other}, device_id_type=MESH,
        ).wait_recv()

    def hand_on(at, mask):
        later = [o for offsets in stages[stage_of[mask] + 1 :] for o in offsets]
        for offset in later + [None]:
            start(at, mask, offset)

    def forward(at, masks):
        for mask in masks:
            arrived(at, mask)
            hand_on(at, mask)

    hand_on(0, 0)
    hand_on(1, 0)
    waits = sorted(range(1, chips), key=lambda m: (bin(m).count("1"), -m))
    far = waits[:1]
    near = [mask for mask in waits if mask in greeted and mask not in far]
    relayed = [mask for mask in waits if mask not in greeted]

    per = LANES // dirs
    lane = lax.broadcasted_iota(jnp.int32, (1, LANES), 1)
    group = lane // dirs
    k_rows = []
    dir_row = jnp.zeros((1, LANES), jnp.int32)
    for axis in range(3):
        k_rows.append(jnp.zeros((1, LANES), F32))
    for d in range(dirs):
        here = lane % dirs == d
        index = dir_s[d]
        dir_row = jnp.where(here, index, dir_row)
        for axis in range(3):
            k_rows[axis] = jnp.where(here, wave_s[axis, index], k_rows[axis])

    def block_of(j):
        order = jnp.zeros((1, LANES), jnp.int32)
        for g in range(per):
            order = jnp.where(group == g, ORDER[j][g], order)
        return order

    orders = [block_of(j) for j in range(BLOCK)]
    steps = blocks // per
    tiles = [(q, j) for q in range(steps) for j in range(BLOCK)]
    sphere_at = jnp.concatenate([(orders[j] + q * per) * BLOCK + j for q, j in tiles], 0)
    here = [jnp.zeros((len(tiles), LANES), F32) for _ in range(3)]
    for s in range(spheres):
        mine = sphere_at == s
        for axis in range(3):
            here[axis] = jnp.where(mine, pos_s[axis, s], here[axis])

    def phase_of(x, y, z):
        return sincos(x * k_rows[0] + y * k_rows[1] + z * k_rows[2])

    own_c, own_s = phase_of(*here)
    own_e[0] = own_c
    own_e[1] = own_s

    def prepare_table():
        load_table.wait()
        for c in range(0, classes, 2):
            at = pl.ds(c * modes, 2 * modes)
            real = jnp.concatenate([table[c, 0], table[c + 1, 0]], 1)
            imag = jnp.concatenate([table[c, 1], table[c + 1, 1]], 1)
            t_real[:, at] = real
            t_diff[:, at] = imag - real
            t_sum[:, at] = imag + real

    def prepare_field():
        load_pattern.wait()
        tables = pattern.shape[2]
        chosen = (lax.broadcasted_iota(jnp.int32, (tables, LANES), 0) == dir_row).astype(F32).astype(BF16)
        for p in range(2):
            high, rest = split_two(pattern[p])
            pat[p] = jnp.dot(high, chosen, preferred_element_type=F32) + jnp.dot(
                rest, chosen, preferred_element_type=F32
            )
        sphere_id = lax.broadcasted_iota(jnp.int32, (spheres, LANES), 0)
        picks = jnp.concatenate(
            [(sphere_id == sphere_at[t : t + 1]).astype(F32) for t in range(len(tiles))], 1
        )
        picks = jnp.concatenate([picks, picks], 0).astype(BF16)
        for p in range(2):
            pieces = jnp.concatenate(split_two(mie[p]), 0)
            spread[p] = lax.dot_general(
                pieces, picks, (((0,), (0,)), ((), ())), preferred_element_type=F32
            )
        for t in range(len(tiles)):
            at = pl.ds(t * LANES, LANES)
            c, s = own_c[t : t + 1], own_s[t : t + 1]
            inc[0, :, at] = c * pat[0] - s * pat[1]
            inc[1, :, at] = c * pat[1] + s * pat[0]

    forward(0, far)
    forward(1, far)
    prepare_table()
    forward(0, near + relayed)
    forward(1, near)
    prepare_field()
    forward(1, relayed)
    for slot in range(chips):
        arrived(0, chips + slot)

    slot_id = lax.broadcasted_iota(jnp.int32, (slots, devices), 0)
    from_device = (slot_id // capacity == lax.broadcasted_iota(jnp.int32, (slots, devices), 1)).astype(F32)
    lists = jnp.concatenate([all_small[:, r, :] for r in range(8)], 1)
    lists = jnp.dot(from_device, lists, precision=HIGHEST, preferred_element_type=F32)
    slot_row = lax.broadcasted_iota(jnp.int32, (slots, LANES), 0)
    slot_lane = lax.broadcasted_iota(jnp.int32, (slots, LANES), 1)
    wanted = slot_lane == me * capacity + slot_row % capacity
    cols = [
        jnp.sum(jnp.where(wanted, lists[:, r * LANES : (r + 1) * LANES], 0.0), 1, keepdims=True)
        for r in range(8)
    ]
    cell = cols[0].astype(jnp.int32) - 1
    owner = lax.broadcasted_iota(jnp.int32, (slots, 1), 0) // capacity
    row_of = owner * spheres + cols[1].astype(jnp.int32) * BLOCK
    for j in range(BLOCK):
        c, s = phase_of(*cols[2 + 3 * j : 5 + 3 * j])
        phase[j, :slots, :] = c
        phase[j, slots:, :] = s
        delta[j] = cell - orders[j]
    total = devices * spheres
    at_row = lax.broadcasted_iota(jnp.int32, (slots, total), 1)
    pick = jnp.concatenate(
        [(at_row == row_of + j).astype(F32).astype(BF16) for j in range(BLOCK)], 0
    )

    for slot in range(chips):
        arrived(1, chips + slot)
    gathered = jnp.dot(
        pick, all_mie[...].reshape(total, 2 * modes), preferred_element_type=F32
    )
    for j in range(BLOCK):
        turned = gathered[j * slots : (j + 1) * slots].T.astype(BF16)
        real, imag = turned[:modes], turned[modes:]
        for g in range(PARTS):
            piece = slice(g * chunk, (g + 1) * chunk)
            upper = pl.ds(2 * g * chunk, chunk)
            lower = pl.ds((2 * g + 1) * chunk, chunk)
            weights[j, upper, :slots] = real[piece]
            weights[j, upper, slots:] = -imag[piece]
            weights[j, lower, :slots] = imag[piece]
            weights[j, lower, slots:] = real[piece]

    width = BLOCK * LANES

    def build(q):
        work = []
        for c in range(0, classes, 2):
            for j in range(BLOCK):
                c_all, s_all = phase[j, :slots, :], phase[j, slots:, :]
                tops, bottoms = [], []
                for h in range(2):
                    here = delta[j] == (c + h) * blocks + q * per
                    tops.append(jnp.where(here, c_all, 0.0))
                    bottoms.append(jnp.where(here, s_all, 0.0))
                masked = jnp.concatenate(
                    [jnp.concatenate(tops, 1), jnp.concatenate(bottoms, 1)], 0
                ).astype(BF16)
                for g in range(PARTS):
                    work.append(functools.partial(piece_of, q, j, c, g, masked))
        return work

    def piece_of(q, j, c, g, masked):
        both = pl.ds(2 * g * chunk, 2 * chunk)
        y = jnp.dot(weights[j, both, :], masked, preferred_element_type=F32)
        own = pl.ds(g * chunk, chunk)
        pr, pi = pat[0, own, :], pat[1, own, :]
        for h in range(2):
            at = slice(h * LANES, (h + 1) * LANES)
            yr, yi = y[:chunk, at], y[chunk:, at]
            mr = yr * pr - yi * pi
            mi = yr * pi + yi * pr
            rows = pl.ds((c + h) * modes + g * chunk, chunk)
            lanes = pl.ds(j * LANES, LANES)
            x_real[q % 2, rows, lanes] = mr.astype(BF16)
            x_imag[q % 2, rows, lanes] = mi.astype(BF16)
            x_sum[q % 2, rows, lanes] = (mr + mi).astype(BF16)

    def finish(q, begin, count, both, first, second):
        at = pl.ds(q * width, width)
        own = pl.ds(begin, count)
        inc_r, inc_i = inc[0, own, at], inc[1, own, at]
        total_r = inc_r + (both - second)
        total_i = inc_i + (both + first)
        mr, mi = spread[0, own, at], spread[1, own, at]
        out_r = mr * total_r - mi * total_i
        out_i = mr * total_i + mi * total_r
        terms = inc_r * out_r + inc_i * out_i
        terms = jnp.sum(terms.reshape(count // 8, 8, width), 0)
        part[...] += terms[:, :LANES] + terms[:, LANES:]
        even = (lax.broadcasted_iota(jnp.int32, (count, LANES), 1) // dirs) % 2 == 0
        for p, out in ((0, out_r), (1, out_i)):
            left, right = out[:, :LANES], out[:, LANES:]
            head = jnp.where(even, left, right)
            tail = pltpu.roll(jnp.where(even, right, left), LANES - dirs, 1)
            rows = pl.ds(p * modes + begin, count)
            scattered[rows, pl.ds(q * width, LANES)] = head.astype(BF16)
            scattered[rows, pl.ds(q * width + LANES, LANES)] = tail.astype(BF16)

    part[...] = jnp.zeros_like(part)
    pairs_of = ((t_real, x_sum), (t_diff, x_real), (t_sum, x_imag))
    deep = classes * modes // DEPTH
    values = {}

    def multiply(q, n, i, rows=slice(0, modes)):
        matrix, mixed = pairs_of[n]
        at = slice(i * DEPTH, (i + 1) * DEPTH)
        term = jnp.dot(matrix[rows, at], mixed[q % 2, at, :], preferred_element_type=F32)
        values[n] = values[n] + term if i else term

    first = build(0)
    begun = [0] * 3
    for n, work in enumerate(first):
        work()
        ready = (n + 1) * classes // len(first) * modes if (n + 1) % (len(first) * 2 // classes) == 0 else 0
        for m in range(1):
            while (begun[m] + 1) * DEPTH <= ready:
                multiply(0, m, begun[m])
                begun[m] += 1
    for q in range(steps):
        todo = build(q + 1) if q + 1 < steps else []
        done = 0
        count = modes // SPLIT if 0 < q == steps - 1 else modes
        for begin in range(0, modes, count):
            rest = [(n, i) for n in range(3) for i in range(begun[n], deep)]
            for at, (n, i) in enumerate(rest):
                multiply(q, n, i, slice(begin, begin + count))
                while done < (at + 1) * len(todo) // len(rest):
                    todo[done]()
                    done += 1
            begun = [0] * 3
            finish(q, begin, count, *(values[n] for n in range(3)))

    row = jnp.sum(part[...], 0, keepdims=True)
    part[0:1, :] = row
    sends = []
    for r, peer in enumerate(everyone):
        copy = pltpu.make_async_remote_copy(
            src_ref=part.at[pl.ds(0, 1)], dst_ref=inbox.at[me], send_sem=ext_send.at[r], recv_sem=ext_recv.at[r],
            device_id={"sph": peer}, device_id_type=MESH,
        )
        copy.start()
        sends.append(copy)
    inbox[me] = row
    for copy in copies[0] + copies[1]:
        copy.wait_send()
    for copy in sends:
        copy.wait_recv()
    row = jnp.sum(inbox[...], 0)
    shift = LANES // 2
    while shift >= dirs:
        row = row + pltpu.roll(row, shift, 1)
        shift //= 2
    ext[...] = row
    for copy in sends:
        copy.wait_send()


def shards(
    positions, wave_vectors, pattern, dir_index, mie, trans_table, pair_route, pair_source,
    pair_target, pair_class,
):
    modes = pattern.shape[1]
    spheres = positions.shape[0]
    dirs = dir_index.shape[0]
    blocks = spheres // BLOCK
    classes = trans_table.shape[0]
    devices = lax.axis_size("sph")
    pair_count = pair_source.shape[0]
    capacity = max(2, 2 * pair_count // devices)
    slots = devices * capacity
    chips = devices // 2
    bits = chips.bit_length() - 1
    per = LANES // dirs
    steps = blocks // per
    width = BLOCK * LANES
    depth = classes * modes
    columns = steps * width
    assert modes % (16 * PARTS) == 0 and depth % DEPTH == 0 and classes % 2 == 0
    assert chips == 1 << bits and slots == LANES and per == len(ORDER[0]) and BLOCK == len(ORDER)

    vmem = pl.BlockSpec(memory_space=pltpu.VMEM)
    dims = (modes, dirs, spheres, blocks, classes, devices, capacity)
    dma = pltpu.SemaphoreType.DMA
    scattered, ext = pl.pallas_call(
        functools.partial(fused_kernel, dims),
        out_shape=[
            jax.ShapeDtypeStruct((2 * modes, columns), BF16),
            jax.ShapeDtypeStruct((1, LANES), F32),
        ],
        in_specs=[pl.BlockSpec(memory_space=pltpu.HBM)] * 10,
        out_specs=[vmem, vmem],
        scratch_shapes=[
            pltpu.VMEM((1, pair_count), jnp.int32),
            pltpu.VMEM((1, pair_count), jnp.int32),
            pltpu.VMEM((1, pair_count), jnp.int32),
            pltpu.VMEM((1, pair_count), jnp.int32),
            pltpu.SMEM((3, spheres), F32),
            pltpu.VMEM((3, spheres), F32),
            pltpu.SMEM((3, wave_vectors.shape[0]), F32),
            pltpu.SMEM((dirs,), jnp.int32),
            pltpu.VMEM((2, spheres, modes), F32),
            pltpu.VMEM(trans_table.shape, BF16),
            pltpu.VMEM(pattern.shape, F32),
            pltpu.VMEM((modes, depth), BF16),
            pltpu.VMEM((modes, depth), BF16),
            pltpu.VMEM((modes, depth), BF16),
            pltpu.VMEM((devices, spheres, 2 * modes), BF16),
            pltpu.VMEM((devices, 8, LANES), F32),
            pltpu.VMEM((BLOCK, 2 * modes, 2 * slots), BF16),
            pltpu.VMEM((2, depth, width), BF16),
            pltpu.VMEM((2, depth, width), BF16),
            pltpu.VMEM((2, depth, width), BF16),
            pltpu.VMEM((2, modes, LANES), F32),
            pltpu.VMEM((2, modes, columns), F32),
            pltpu.VMEM((2, modes, columns), F32),
            pltpu.VMEM((2, steps * BLOCK, LANES), F32),
            pltpu.VMEM((BLOCK, 2 * slots, LANES), F32),
            pltpu.VMEM((BLOCK, slots, LANES), jnp.int32),
            pltpu.VMEM((8, LANES), F32),
            pltpu.VMEM((devices, 1, LANES), F32),
            dma((11,)),
            dma((2, 2 * chips)),
            dma((2, 2 * chips)),
            dma((devices,)),
            dma((devices,)),
        ],
        compiler_params=pltpu.CompilerParams(
            collective_id=0, has_side_effects=True, vmem_limit_bytes=48 * 1024 * 1024
        ),
        name="fused",
    )(
        *[pltpu.with_memory_space_constraint(x, pltpu.HBM) for x in (
        pair_route.reshape(1, pair_count), pair_source.reshape(1, pair_count),
        pair_target.reshape(1, pair_count), pair_class.reshape(1, pair_count),
        positions.T, wave_vectors.T, dir_index, jnp.transpose(mie, (0, 2, 1)),
        pattern, trans_table,
        )]
    )
    return scattered, ext[0, :dirs]


def solution(mesh):
    placed = (
        P("sph", None), P(), P(), P("groups"), P(None, None, "sph"), P(),
        P("sph", None), P("sph"), P("sph"), P("sph"),
    )
    return jax.shard_map(
        shards,
        mesh=mesh,
        in_specs=placed,
        out_specs=(P(None, ("groups", "sph")), P("groups")),
        check_vma=False,
    )
```

```python
import functools

import jax
import jax.numpy as jnp
from jax import lax
from jax.experimental import pallas as pl
from jax.experimental.pallas import tpu as pltpu
from jax.sharding import PartitionSpec as P

BLOCK = 2
LANES = 128
HIGHEST = lax.Precision.HIGHEST
MESH = pl.DeviceIdType.MESH
F32 = jnp.float32
BF16 = jnp.bfloat16
ORDER = ((0, 2, 1, 3), (3, 0, 2, 1))
PARTS = 4
DEPTH = 512
SPLIT = 2


def sincos(angle):
    turns = jnp.floor(angle * 0.6366197723675814 + 0.5)
    rest = angle - turns * 1.5703125
    rest = rest - turns * 4.837512969970703125e-4
    rest = rest - turns * 7.54978995489188216e-8
    square = rest * rest
    sine = rest + rest * square * (
        -1.6666654611e-1 + square * (8.3321608736e-3 + square * -1.9515295891e-4)
    )
    cosine = 1.0 - 0.5 * square + square * square * (
        4.166664568298827e-2 + square * (-1.388731625493765e-3 + square * 2.443315711809948e-5)
    )
    quarter = turns.astype(jnp.int32)
    swap = (quarter & 1) == 1
    c = jnp.where(swap, sine, cosine)
    s = jnp.where(swap, cosine, sine)
    c = jnp.where(((quarter + 1) & 2) == 2, -c, c)
    s = jnp.where((quarter & 2) == 2, -s, s)
    return c, s


def split_two(x):
    high = x.astype(BF16)
    return high, (x - high.astype(F32)).astype(BF16)


def fused_kernel(
    dims, route_hbm, source_hbm, target_hbm, kind_hbm, pos_hbm, wave_hbm, dir_hbm, mie_hbm,
    pattern_hbm, table_hbm, scattered, ext,
    route, source, target, kind, pos_s, pos_v, wave_s, dir_s, mie, table, pattern, t_real, t_diff, t_sum, all_mie, all_small, weights, x_real, x_imag, x_sum,
    pat, inc, spread, own_e, phase, delta, part, inbox,
    loaded, send, recv, ext_send, ext_recv,
):
    modes, dirs, spheres, blocks, classes, devices, capacity = dims
    chunk = modes // PARTS
    me = lax.axis_index("sph")
    chips = devices // 2
    chip, core = me // 2, me % 2
    other = chip * 2 + (1 - core)
    bits = []
    bit = chips // 2
    while bit >= 1:
        bits.append(bit)
        bit //= 2

    def flip(value, bit):
        return value + bit - 2 * bit * ((value // bit) % 2)

    def chip_at(mask):
        value = chip
        for bit in bits:
            if mask & bit:
                value = flip(value, bit)
        return value

    stages = [[bit] for bit in bits[:-2]] + [bits[-2:] + [sum(bits[-2:])] if len(bits) > 1 else bits]
    held, routes = [0], []
    for stage, offsets in enumerate(stages):
        routes.append((list(held), offsets))
        held = held + [h | o for o in offsets for h in held]
    stage_of = {0: -1}
    for stage, (before, offsets) in enumerate(routes):
        for o in offsets:
            for h in before:
                stage_of[h | o] = stage
    greeted = [o for offsets in stages for o in offsets]
    partners = [chip_at(o) * 2 + core for o in greeted] + [other]
    everyone = [(me + r) % devices for r in range(1, devices)]

    barrier = pltpu.get_barrier_semaphore()
    for peer in partners:
        pl.semaphore_signal(barrier, inc=1, device_id={"sph": peer}, device_id_type=MESH)
    load_table = pltpu.make_async_copy(table_hbm, table, loaded.at[0])
    load_pattern = pltpu.make_async_copy(pattern_hbm, pattern, loaded.at[1])
    small = (
        (route_hbm, route), (source_hbm, source), (target_hbm, target), (kind_hbm, kind),
        (pos_hbm, pos_v), (mie_hbm, mie), (pos_hbm, pos_s), (wave_hbm, wave_s), (dir_hbm, dir_s),
    )
    fetches = [pltpu.make_async_copy(a, b, loaded.at[2 + i]) for i, (a, b) in enumerate(small)]
    for copy in fetches:
        copy.start()
    load_pattern.start()
    load_table.start()
    for copy in fetches:
        copy.wait()

    pairs = route.shape[1]
    slots = devices * capacity
    ia = lax.broadcasted_iota(jnp.int32, (pairs, pairs), 0)
    ib = lax.broadcasted_iota(jnp.int32, (pairs, pairs), 1)

    def column(row):
        return jnp.sum(jnp.where(ia == ib, row, 0.0), 1, keepdims=True)

    dest = route[...].astype(F32)
    dest_col = column(dest)
    rank = jnp.sum(jnp.where((dest_col == dest) & (ib < ia), 1.0, 0.0), 1, keepdims=True)
    slot_lane = lax.broadcasted_iota(jnp.int32, (pairs, LANES), 1).astype(F32)
    match = (dest_col * capacity + rank) == slot_lane
    source_col = column(source[...].astype(F32))
    cell_col = column((kind[...] * blocks + target[...] + 1).astype(F32))
    sphere_lane = lax.broadcasted_iota(jnp.int32, (pairs, spheres), 1).astype(F32)
    entries = [cell_col, source_col]
    for j in range(BLOCK):
        picked = sphere_lane == source_col * BLOCK + j
        for axis in range(3):
            entries.append(
                jnp.sum(jnp.where(picked, pos_v[axis : axis + 1, :], 0.0), 1, keepdims=True)
            )
    rows = [jnp.sum(jnp.where(match, entry, 0.0), 0, keepdims=True) for entry in entries]
    all_small[me] = jnp.concatenate(rows, 0)
    all_mie[me] = jnp.concatenate([mie[0], mie[1]], 1).astype(BF16)

    pl.semaphore_wait(barrier, len(partners))

    copies = ([], [])
    items = (all_small, all_mie)

    def start(at, mask, offset):
        ref = items[at].at[chip_at(mask) * 2 + core]
        slot = chips + mask if offset is None else mask | offset
        target = other if offset is None else chip_at(offset) * 2 + core
        copy = pltpu.make_async_remote_copy(
            src_ref=ref, dst_ref=ref, send_sem=send.at[at, len(copies[at])],
            recv_sem=recv.at[at, slot], device_id={"sph": target}, device_id_type=MESH,
        )
        copy.start()
        copies[at].append(copy)

    def arrived(at, slot):
        ref = items[at].at[me]
        pltpu.make_async_remote_copy(
            src_ref=ref, dst_ref=ref, send_sem=send.at[at, 0], recv_sem=recv.at[at, slot],
            device_id={"sph": other}, device_id_type=MESH,
        ).wait_recv()

    def hand_on(at, mask):
        later = [o for offsets in stages[stage_of[mask] + 1 :] for o in offsets]
        for offset in later + [None]:
            start(at, mask, offset)

    def forward(at, masks):
        for mask in masks:
            arrived(at, mask)
            hand_on(at, mask)

    hand_on(0, 0)
    hand_on(1, 0)
    waits = sorted(range(1, chips), key=lambda m: (bin(m).count("1"), -m))
    far = waits[:1]
    near = [mask for mask in waits if mask in greeted and mask not in far]
    relayed = [mask for mask in waits if mask not in greeted]

    per = LANES // dirs
    lane = lax.broadcasted_iota(jnp.int32, (1, LANES), 1)
    group = lane // dirs
    k_rows = []
    dir_row = jnp.zeros((1, LANES), jnp.int32)
    for axis in range(3):
        k_rows.append(jnp.zeros((1, LANES), F32))
    for d in range(dirs):
        here = lane % dirs == d
        index = dir_s[d]
        dir_row = jnp.where(here, index, dir_row)
        for axis in range(3):
            k_rows[axis] = jnp.where(here, wave_s[axis, index], k_rows[axis])

    def block_of(j):
        order = jnp.zeros((1, LANES), jnp.int32)
        for g in range(per):
            order = jnp.where(group == g, ORDER[j][g], order)
        return order

    orders = [block_of(j) for j in range(BLOCK)]
    steps = blocks // per
    tiles = [(q, j) for q in range(steps) for j in range(BLOCK)]
    sphere_at = jnp.concatenate([(orders[j] + q * per) * BLOCK + j for q, j in tiles], 0)
    here = [jnp.zeros((len(tiles), LANES), F32) for _ in range(3)]
    for s in range(spheres):
        mine = sphere_at == s
        for axis in range(3):
            here[axis] = jnp.where(mine, pos_s[axis, s], here[axis])

    def phase_of(x, y, z):
        return sincos(x * k_rows[0] + y * k_rows[1] + z * k_rows[2])

    own_c, own_s = phase_of(*here)
    own_e[0] = own_c
    own_e[1] = own_s

    def prepare_table():
        load_table.wait()
        for c in range(0, classes, 2):
            at = pl.ds(c * modes, 2 * modes)
            real = jnp.concatenate([table[c, 0], table[c + 1, 0]], 1)
            imag = jnp.concatenate([table[c, 1], table[c + 1, 1]], 1)
            t_real[:, at] = real
            t_diff[:, at] = imag - real
            t_sum[:, at] = imag + real

    def prepare_field():
        load_pattern.wait()
        tables = pattern.shape[2]
        chosen = (lax.broadcasted_iota(jnp.int32, (tables, LANES), 0) == dir_row).astype(F32).astype(BF16)
        for p in range(2):
            high, rest = split_two(pattern[p])
            pat[p] = jnp.dot(high, chosen, preferred_element_type=F32) + jnp.dot(
                rest, chosen, preferred_element_type=F32
            )
        sphere_id = lax.broadcasted_iota(jnp.int32, (spheres, LANES), 0)
        picks = jnp.concatenate(
            [(sphere_id == sphere_at[t : t + 1]).astype(F32) for t in range(len(tiles))], 1
        )
        picks = jnp.concatenate([picks, picks], 0).astype(BF16)
        for p in range(2):
            pieces = jnp.concatenate(split_two(mie[p]), 0)
            spread[p] = lax.dot_general(
                pieces, picks, (((0,), (0,)), ((), ())), preferred_element_type=F32
            )
        for t in range(len(tiles)):
            at = pl.ds(t * LANES, LANES)
            c, s = own_c[t : t + 1], own_s[t : t + 1]
            inc[0, :, at] = c * pat[0] - s * pat[1]
            inc[1, :, at] = c * pat[1] + s * pat[0]

    forward(0, far)
    forward(1, far)
    prepare_table()
    forward(0, near + relayed)
    forward(1, near)
    prepare_field()
    forward(1, relayed)
    for slot in range(chips):
        arrived(0, chips + slot)

    slot_id = lax.broadcasted_iota(jnp.int32, (slots, devices), 0)
    from_device = (slot_id // capacity == lax.broadcasted_iota(jnp.int32, (slots, devices), 1)).astype(F32)
    lists = jnp.concatenate([all_small[:, r, :] for r in range(8)], 1)
    lists = jnp.dot(from_device, lists, precision=HIGHEST, preferred_element_type=F32)
    slot_row = lax.broadcasted_iota(jnp.int32, (slots, LANES), 0)
    slot_lane = lax.broadcasted_iota(jnp.int32, (slots, LANES), 1)
    wanted = slot_lane == me * capacity + slot_row % capacity
    cols = [
        jnp.sum(jnp.where(wanted, lists[:, r * LANES : (r + 1) * LANES], 0.0), 1, keepdims=True)
        for r in range(8)
    ]
    cell = cols[0].astype(jnp.int32) - 1
    owner = lax.broadcasted_iota(jnp.int32, (slots, 1), 0) // capacity
    row_of = owner * spheres + cols[1].astype(jnp.int32) * BLOCK
    for j in range(BLOCK):
        c, s = phase_of(*cols[2 + 3 * j : 5 + 3 * j])
        phase[j, :slots, :] = c
        phase[j, slots:, :] = s
        delta[j] = cell - orders[j]
    total = devices * spheres
    at_row = lax.broadcasted_iota(jnp.int32, (slots, total), 1)
    pick = jnp.concatenate(
        [(at_row == row_of + j).astype(F32).astype(BF16) for j in range(BLOCK)], 0
    )

    for slot in range(chips):
        arrived(1, chips + slot)
    gathered = jnp.dot(
        pick, all_mie[...].reshape(total, 2 * modes), preferred_element_type=F32
    )
    for j in range(BLOCK):
        turned = gathered[j * slots : (j + 1) * slots].astype(BF16).T
        real, imag = turned[:modes], turned[modes:]
        for g in range(PARTS):
            piece = slice(g * chunk, (g + 1) * chunk)
            upper = pl.ds(2 * g * chunk, chunk)
            lower = pl.ds((2 * g + 1) * chunk, chunk)
            weights[j, upper, :slots] = real[piece]
            weights[j, upper, slots:] = -imag[piece]
            weights[j, lower, :slots] = imag[piece]
            weights[j, lower, slots:] = real[piece]

    width = BLOCK * LANES

    def build(q):
        work = []
        for c in range(0, classes, 2):
            for j in range(BLOCK):
                c_all, s_all = phase[j, :slots, :], phase[j, slots:, :]
                tops, bottoms = [], []
                for h in range(2):
                    here = delta[j] == (c + h) * blocks + q * per
                    tops.append(jnp.where(here, c_all, 0.0))
                    bottoms.append(jnp.where(here, s_all, 0.0))
                masked = jnp.concatenate(
                    [jnp.concatenate(tops, 1), jnp.concatenate(bottoms, 1)], 0
                ).astype(BF16)
                for g in range(PARTS):
                    work.append(functools.partial(piece_of, q, j, c, g, masked))
        return work

    def piece_of(q, j, c, g, masked):
        both = pl.ds(2 * g * chunk, 2 * chunk)
        y = jnp.dot(weights[j, both, :], masked, preferred_element_type=F32)
        own = pl.ds(g * chunk, chunk)
        pr, pi = pat[0, own, :], pat[1, own, :]
        for h in range(2):
            at = slice(h * LANES, (h + 1) * LANES)
            yr, yi = y[:chunk, at], y[chunk:, at]
            mr = yr * pr - yi * pi
            mi = yr * pi + yi * pr
            rows = pl.ds((c + h) * modes + g * chunk, chunk)
            lanes = pl.ds(j * LANES, LANES)
            x_real[q % 2, rows, lanes] = mr.astype(BF16)
            x_imag[q % 2, rows, lanes] = mi.astype(BF16)
            x_sum[q % 2, rows, lanes] = (mr + mi).astype(BF16)

    def finish(q, begin, count, both, first, second):
        at = pl.ds(q * width, width)
        own = pl.ds(begin, count)
        inc_r, inc_i = inc[0, own, at], inc[1, own, at]
        total_r = inc_r + (both - second)
        total_i = inc_i + (both + first)
        mr, mi = spread[0, own, at], spread[1, own, at]
        out_r = mr * total_r - mi * total_i
        out_i = mr * total_i + mi * total_r
        terms = inc_r * out_r + inc_i * out_i
        terms = jnp.sum(terms.reshape(count // 8, 8, width), 0)
        part[...] += terms[:, :LANES] + terms[:, LANES:]
        even = (lax.broadcasted_iota(jnp.int32, (count, LANES), 1) // dirs) % 2 == 0
        for p, out in ((0, out_r), (1, out_i)):
            left, right = out[:, :LANES], out[:, LANES:]
            head = jnp.where(even, left, right)
            tail = pltpu.roll(jnp.where(even, right, left), LANES - dirs, 1)
            rows = pl.ds(p * modes + begin, count)
            scattered[rows, pl.ds(q * width, LANES)] = head.astype(BF16)
            scattered[rows, pl.ds(q * width + LANES, LANES)] = tail.astype(BF16)

    part[...] = jnp.zeros_like(part)
    pairs_of = ((t_real, x_sum), (t_diff, x_real), (t_sum, x_imag))
    deep = classes * modes // DEPTH
    values = {}

    def multiply(q, n, i, rows=slice(0, modes)):
        matrix, mixed = pairs_of[n]
        at = slice(i * DEPTH, (i + 1) * DEPTH)
        term = jnp.dot(matrix[rows, at], mixed[q % 2, at, :], preferred_element_type=F32)
        values[n] = values[n] + term if i else term

    first = build(0)
    begun = [0] * 3
    for n, work in enumerate(first):
        work()
        ready = (n + 1) * classes // len(first) * modes if (n + 1) % (len(first) * 2 // classes) == 0 else 0
        for m in range(1):
            while (begun[m] + 1) * DEPTH <= ready:
                multiply(0, m, begun[m])
                begun[m] += 1
    for q in range(steps):
        todo = build(q + 1) if q + 1 < steps else []
        done = 0
        count = modes // SPLIT if 0 < q == steps - 1 else modes
        for begin in range(0, modes, count):
            rest = [(n, i) for n in range(3) for i in range(begun[n], deep)]
            for at, (n, i) in enumerate(rest):
                multiply(q, n, i, slice(begin, begin + count))
                while done < (at + 1) * len(todo) // len(rest):
                    todo[done]()
                    done += 1
            begun = [0] * 3
            finish(q, begin, count, *(values[n] for n in range(3)))

    row = jnp.sum(part[...], 0, keepdims=True)
    part[0:1, :] = row
    sends = []
    for r, peer in enumerate(everyone):
        copy = pltpu.make_async_remote_copy(
            src_ref=part.at[pl.ds(0, 1)], dst_ref=inbox.at[me], send_sem=ext_send.at[r], recv_sem=ext_recv.at[r],
            device_id={"sph": peer}, device_id_type=MESH,
        )
        copy.start()
        sends.append(copy)
    inbox[me] = row
    for copy in copies[0] + copies[1]:
        copy.wait_send()
    for copy in sends:
        copy.wait_recv()
    row = jnp.sum(inbox[...], 0)
    shift = LANES // 2
    while shift >= dirs:
        row = row + pltpu.roll(row, shift, 1)
        shift //= 2
    ext[...] = row
    for copy in sends:
        copy.wait_send()


def shards(
    positions, wave_vectors, pattern, dir_index, mie, trans_table, pair_route, pair_source,
    pair_target, pair_class,
):
    modes = pattern.shape[1]
    spheres = positions.shape[0]
    dirs = dir_index.shape[0]
    blocks = spheres // BLOCK
    classes = trans_table.shape[0]
    devices = lax.axis_size("sph")
    pair_count = pair_source.shape[0]
    capacity = max(2, 2 * pair_count // devices)
    slots = devices * capacity
    chips = devices // 2
    bits = chips.bit_length() - 1
    per = LANES // dirs
    steps = blocks // per
    width = BLOCK * LANES
    depth = classes * modes
    columns = steps * width
    assert modes % (16 * PARTS) == 0 and depth % DEPTH == 0 and classes % 2 == 0
    assert chips == 1 << bits and slots == LANES and per == len(ORDER[0]) and BLOCK == len(ORDER)

    vmem = pl.BlockSpec(memory_space=pltpu.VMEM)
    dims = (modes, dirs, spheres, blocks, classes, devices, capacity)
    dma = pltpu.SemaphoreType.DMA
    scattered, ext = pl.pallas_call(
        functools.partial(fused_kernel, dims),
        out_shape=[
            jax.ShapeDtypeStruct((2 * modes, columns), BF16),
            jax.ShapeDtypeStruct((1, LANES), F32),
        ],
        in_specs=[pl.BlockSpec(memory_space=pltpu.HBM)] * 10,
        out_specs=[vmem, vmem],
        scratch_shapes=[
            pltpu.VMEM((1, pair_count), jnp.int32),
            pltpu.VMEM((1, pair_count), jnp.int32),
            pltpu.VMEM((1, pair_count), jnp.int32),
            pltpu.VMEM((1, pair_count), jnp.int32),
            pltpu.SMEM((3, spheres), F32),
            pltpu.VMEM((3, spheres), F32),
            pltpu.SMEM((3, wave_vectors.shape[0]), F32),
            pltpu.SMEM((dirs,), jnp.int32),
            pltpu.VMEM((2, spheres, modes), F32),
            pltpu.VMEM(trans_table.shape, BF16),
            pltpu.VMEM(pattern.shape, F32),
            pltpu.VMEM((modes, depth), BF16),
            pltpu.VMEM((modes, depth), BF16),
            pltpu.VMEM((modes, depth), BF16),
            pltpu.VMEM((devices, spheres, 2 * modes), BF16),
            pltpu.VMEM((devices, 8, LANES), F32),
            pltpu.VMEM((BLOCK, 2 * modes, 2 * slots), BF16),
            pltpu.VMEM((2, depth, width), BF16),
            pltpu.VMEM((2, depth, width), BF16),
            pltpu.VMEM((2, depth, width), BF16),
            pltpu.VMEM((2, modes, LANES), F32),
            pltpu.VMEM((2, modes, columns), F32),
            pltpu.VMEM((2, modes, columns), F32),
            pltpu.VMEM((2, steps * BLOCK, LANES), F32),
            pltpu.VMEM((BLOCK, 2 * slots, LANES), F32),
            pltpu.VMEM((BLOCK, slots, LANES), jnp.int32),
            pltpu.VMEM((8, LANES), F32),
            pltpu.VMEM((devices, 1, LANES), F32),
            dma((11,)),
            dma((2, 2 * chips)),
            dma((2, 2 * chips)),
            dma((devices,)),
            dma((devices,)),
        ],
        compiler_params=pltpu.CompilerParams(
            collective_id=0, has_side_effects=True, vmem_limit_bytes=48 * 1024 * 1024
        ),
        name="fused",
    )(
        *[pltpu.with_memory_space_constraint(x, pltpu.HBM) for x in (
        pair_route.reshape(1, pair_count), pair_source.reshape(1, pair_count),
        pair_target.reshape(1, pair_count), pair_class.reshape(1, pair_count),
        positions.T, wave_vectors.T, dir_index, jnp.transpose(mie, (0, 2, 1)),
        pattern, trans_table,
        )]
    )
    return scattered, ext[0, :dirs]


def solution(mesh):
    placed = (
        P("sph", None), P(), P(), P("groups"), P(None, None, "sph"), P(),
        P("sph", None), P("sph"), P("sph"), P("sph"),
    )
    return jax.shard_map(
        shards,
        mesh=mesh,
        in_specs=placed,
        out_specs=(P(None, ("groups", "sph")), P("groups")),
        check_vma=False,
    )
```
